128 devices in a mesh: grp: 4 (over y), sub: 32 (over x, z, core).
Axes of the slice: x: 4, y: 4, z: 4, core: 2. Of those that a mesh axis runs over, the one named last changes fastest.
Arguments:
- initial_field: float32 [4, 64, 16384], P('grp', 'sub'), may hold values from -6 to 6
- conduct: float32 [4, 64, 16384], P('grp', 'sub'), may hold values from 0.02 to 0.12
- velocity: float32 [4, 64, 16384], P('grp', 'sub'), may hold values from 0 to 0.25
- heat_release: float32 [4, 64, 16384], P('grp', 'sub'), may hold values from 0.01 to 0.1
- group_kind: int32 [4], replicated, may hold values from 0 to 1, as said below
- partner: int32 [4], replicated, may hold values from 0 to 3, as said below
- surface_cell: int32 [4, 16384], P('grp', 'sub'), may hold values from 0 to 32767
- patch_count: int32 [4, 32], P('grp'), may hold values from 1 to 24, 256 in all within a row
- patch_centres: int32 [4, 768, 128], P('grp', 'sub'), may hold values from 0 to 16383, as said below
- patch_targets: int32 [4, 768, 128], P('grp', 'sub'), may hold values from 0 to 16383
- patch_maps: float32 [4, 768, 128, 128], P('grp', 'sub'), may hold values from -0.25 to 0.95
Outputs:
- temperature: float32 [4, 64, 16384], P('grp', 'sub')
- interface: float32 [4, 2, 16384], P('grp', None, 'sub')
The draws below stay inside these ranges and needn't reach their ends.
Inputs may be any that keep to these rules, and one draw needn't show every extreme that they name: `group_kind`: both kinds occur. partner[g] is a group of the other kind than g. Slots 0 to patch_count[g, j] - 1 of device j of group g are live; each group's counts sum to 256; in each group some device holds 24. `patch_centres`: the centres of slot s of group g lie in the cyclic window of 1024 consecutive nodes that starts at (s // 24) * 512 - 512 // 2 + h[g], for one shift h[g] of each group.
All inputs are finite; a program needn't handle non-finite values.
Results may differ from the reference program's by a relative error of at most 0.00013.
Values sent between devices are 32-bit elements; how exact they have to be, the bound alone decides.
No kernel may reach another device: no remote copies, remote signals or barrier semaphores. Data moves between devices by JAX's collectives and lax.ppermute only.
A program may use at most 64 MiB of HBM per device.

```python
import math
import jax
import jax.numpy as jnp
import numpy as np
from jax import lax

PLANES = 2
CELLS = 16384
SURF_DEV = 512
PATCH = 128
STEPS = 4
COUPLE = 4
GROUPS = 4
STACK = 64
NODES = 16384
CAP = 24
SLOTS = 768
PATCH_ROW = 256
N_SUB = 32


def kinds_partners(key):
    base_key = jax.random.fold_in(key, 17)
    order_key, count_key, score_key = jax.random.split(base_key, 3)
    shuffled = jax.random.permutation(order_key, GROUPS)
    gas_count = jax.random.randint(count_key, (), 1, GROUPS)
    position = jnp.argsort(shuffled, stable=True)
    kinds = (position >= gas_count).astype(jnp.int32)
    scores = jax.random.randint(score_key, (GROUPS, GROUPS), 0, 1000) * GROUPS + jnp.arange(GROUPS)[None, :]
    scores = scores + (kinds[:, None] == kinds[None, :]).astype(jnp.int32) * 1000000
    partners = jnp.argsort(scores, axis=1, stable=True)[:, 0].astype(jnp.int32)
    return (kinds, partners)


def draw_group_kind(key, part):
    return kinds_partners(key)[0]


def draw_partner(key, part):
    return kinds_partners(key)[1]


def window_nodes(key, group_shift):
    owner = (jnp.arange(SLOTS, dtype=jnp.int32) // CAP)[None, :, None]
    start = owner * SURF_DEV - SURF_DEV // 2 + group_shift[:, None, None]
    offset = jax.random.randint(key, (GROUPS, SLOTS, PATCH), 0, 2 * SURF_DEV)
    return ((start + offset) % NODES).astype(jnp.int32)


def draw_patch_targets(key, part):
    target_key = jax.random.fold_in(key, 31)
    return jax.random.randint(target_key, (GROUPS, SLOTS, PATCH), 0, NODES).astype(jnp.int32)


def draw_patch_centres(key, part):
    centre_key = jax.random.fold_in(key, 47)
    shift_key, node_key = jax.random.split(centre_key)
    group_shift = jax.random.randint(shift_key, (GROUPS,), 0, NODES)
    return window_nodes(node_key, group_shift)


def draw_patch_maps(key, part):
    off_key, diag_key = jax.random.split(key)
    full_shape = (GROUPS, SLOTS, PATCH, PATCH)
    spread = jax.random.normal(off_key, full_shape, jnp.float32) * (0.5 / math.sqrt(PATCH))
    spread = jnp.clip(spread, -0.25, 0.25)
    diagonal = jax.random.uniform(diag_key, (GROUPS, SLOTS, PATCH), jnp.float32, 0.3, 0.7)
    return spread + diagonal[..., None] * jnp.eye(PATCH, dtype=jnp.float32)


def set_ends(result, own_key, low, top_value):
    longest = result.shape.index(max(result.shape))
    spots = []
    for shift in (0, 1):
        where = [jax.random.randint(jax.random.fold_in(own_key, axis), (), 0, length) for axis, length in enumerate(result.shape)]
        where[longest] = (where[longest] + shift) % result.shape[longest]
        spots.append(tuple(where))
    return result.at[spots[0]].set(low).at[spots[1]].set(top_value)


def steps_of(key, dims, cuts, low, high):
    loudness, own = 1.0, jax.random.fold_in(key, 6)
    for axis_at, shards_of in cuts:
        steps = jnp.exp(jax.random.uniform(jax.random.fold_in(own, axis_at), (shards_of,), jnp.float32, low / len(cuts), high / len(cuts)))
        loudness = loudness * jnp.repeat(steps, dims[axis_at] // shards_of).reshape([-1 if axis == axis_at else 1 for axis in range(len(dims))])
    return loudness


def length_profile(number_of, total, most, lean):
    weights = [(1 << 20) // math.isqrt(standing ** lean) + 1 for standing in range(2, number_of + 1)]
    spare, holding = total - most - (number_of - 1), [1] * (number_of - 1)
    while spare > 0:
        candidates = [i for i in range(number_of - 1) if holding[i] < most]
        whole, left = sum([weights[i] for i in candidates]), spare
        for i in candidates:
            addition = min(most - holding[i], max(1, left * weights[i] // whole), spare)
            holding[i] = holding[i] + addition
            spare = spare - addition
    return np.array([most] + holding)


def ragged(own_key, count, total, limit, slope):
    if count == 2:
        one = jax.random.randint(own_key, (), max(1, total - limit), min(limit, total - 1) + 1)
        return jnp.stack([one, total - one])
    sizes = jnp.asarray(length_profile(count, total, limit, slope), jnp.int32)
    pairs = (count - 1) // 2
    source_of, sink = sizes[1:1 + 2 * pairs:2], sizes[2:2 + 2 * pairs:2]
    room = jnp.minimum(source_of - 1, limit - sink)
    moved = jax.random.randint(jax.random.fold_in(own_key, 1), (pairs,), 0, 1 << 20) % (room + 1)
    sizes = sizes.at[1:1 + 2 * pairs:2].set(source_of - moved).at[2:2 + 2 * pairs:2].set(sink + moved)
    return sizes[jax.random.permutation(jax.random.fold_in(own_key, 2), count)]


def scatter_about(own_key, dims, deviation, reach, pieces=(), kind=jnp.bfloat16):
    result = deviation * jax.random.normal(own_key, dims, jnp.float32)
    if pieces:
        result = result * steps_of(own_key, dims, pieces, -0.22, 0.18)
    return jnp.clip(result, -reach, reach).astype(kind)


def setup_inputs(seed: int = 0) -> dict:
    key_list = jax.random.split(jax.random.key(seed), 12)
    initial_field = scatter_about(key_list[0], (GROUPS, STACK, CELLS), 1.0, 6.0, ((0, 4), (1, 32)), jnp.float32)
    conduct = jnp.clip(jnp.exp(math.log(0.12) - 1.7917595 * jax.random.uniform(key_list[1], (GROUPS, STACK, CELLS), jnp.float32) ** steps_of(key_list[1], (GROUPS, STACK, CELLS), ((0, 4), (1, 32)), -0.2, 0.2)), 0.02, 0.12)
    velocity = jnp.clip(0.25 * jax.random.uniform(key_list[2], (GROUPS, STACK, CELLS), jnp.float32) ** steps_of(key_list[2], (GROUPS, STACK, CELLS), ((0, 4), (1, 32)), -0.2, 0.2), 0.0, 0.25)
    heat_release = jnp.clip(jnp.exp(math.log(0.1) - 2.3025851 * jax.random.uniform(key_list[3], (GROUPS, STACK, CELLS), jnp.float32) ** steps_of(key_list[3], (GROUPS, STACK, CELLS), ((0, 4), (1, 32)), -0.2, 0.2)), 0.01, 0.1)
    group_kind = draw_group_kind(jax.random.fold_in(key_list[11], 71), 0)
    partner = draw_partner(jax.random.fold_in(key_list[11], 71), 0)
    surface_cell = set_ends(jax.random.randint(key_list[6], (GROUPS, NODES), 0, PLANES * CELLS), jax.random.fold_in(key_list[6], 1), 0, (PLANES * CELLS) - 1).astype(jnp.int32)
    patch_count = jax.vmap(lambda own: ragged(own, N_SUB, PATCH_ROW, CAP, 2))(jax.random.split(key_list[7], GROUPS)).reshape((GROUPS, N_SUB)).astype(jnp.int32)
    patch_centres = draw_patch_centres(jax.random.fold_in(key_list[11], 71), 0)
    patch_targets = draw_patch_targets(jax.random.fold_in(key_list[11], 71), 0)
    patch_maps = draw_patch_maps(jax.random.fold_in(key_list[11], 71), 0)
    return dict(initial_field=initial_field, conduct=conduct, velocity=velocity, heat_release=heat_release, group_kind=group_kind, partner=partner, surface_cell=surface_cell, patch_count=patch_count, patch_centres=patch_centres, patch_targets=patch_targets, patch_maps=patch_maps)


def in_plane(current):
    return (jnp.roll(current, 1, -2) + jnp.roll(current, -1, -2)
            + jnp.roll(current, 1, -1) + jnp.roll(current, -1, -1))


def advance(current, conduct, velocity, heat_release, gas_mask):
    zero_plane = jnp.zeros_like(current[:, :1])
    upper_plane = jnp.concatenate([current[:, 1:], zero_plane], axis=1)
    lower_plane = jnp.concatenate([zero_plane, current[:, :-1]], axis=1)
    laplace = upper_plane + lower_plane + in_plane(current) - 6.0 * current
    return (current + conduct * laplace - gas_mask * velocity * (current - lower_plane)
            + gas_mask * heat_release * jax.nn.sigmoid(2.0 * current))


def reference(initial_field, conduct, velocity, heat_release, group_kind, partner, surface_cell,
              patch_count, patch_centres, patch_targets, patch_maps):
    groups = initial_field.shape[0]
    slab_shape = (groups, N_SUB * PLANES, CELLS // 128, 128)
    current = initial_field.reshape(slab_shape)
    conduct_slab = conduct.reshape(slab_shape)
    velocity_slab = velocity.reshape(slab_shape)
    heat_slab = heat_release.reshape(slab_shape)
    gas_mask = (group_kind == 0).astype(jnp.float32)[:, None, None, None]
    gain_temp = jnp.where(group_kind == 0, 0.5, 0.25).astype(jnp.float32)[:, None]
    gain_flux = jnp.where(group_kind == 0, -0.25, 0.25).astype(jnp.float32)[:, None]
    node_ids = jnp.arange(N_SUB * SURF_DEV, dtype=jnp.int32)
    cell_ids = (node_ids // SURF_DEV)[None, :] * (PLANES * CELLS) + surface_cell
    slot_ids = jnp.arange(N_SUB * CAP, dtype=jnp.int32)
    live_mask = ((slot_ids % CAP)[None, :] < patch_count[:, slot_ids // CAP]).astype(jnp.float32)
    group_ids = jnp.arange(groups, dtype=jnp.int32)[:, None]
    interface = jnp.zeros((groups, 2, N_SUB * SURF_DEV), jnp.float32)
    for iteration in range(COUPLE):
        for substep in range(STEPS):
            current = advance(current, conduct_slab, velocity_slab, heat_slab, gas_mask)
        flux_field = conduct_slab * (4.0 * current - in_plane(current))
        flat_temp = current.reshape(groups, -1)
        flat_flux = flux_field.reshape(groups, -1)
        export = jnp.stack([jnp.take_along_axis(flat_temp, cell_ids, 1),
                            jnp.take_along_axis(flat_flux, cell_ids, 1)], axis=1)
        source = export[partner]
        row_sums = []
        for group in range(groups):
            centre_vals = source[group][:, patch_centres[group]]
            contrib = jnp.einsum("stk,qsk->qst", patch_maps[group], centre_vals,
                                 precision=lax.Precision.HIGHEST) * live_mask[group][None, :, None]
            row_sum = jnp.zeros((2, N_SUB * SURF_DEV), jnp.float32).at[:, patch_targets[group]].add(contrib)
            row_sums.append(row_sum)
        interface = jnp.stack(row_sums)
        increment = gain_temp * (interface[:, 0] - export[:, 0]) + gain_flux * interface[:, 1]
        flat_temp = flat_temp.at[group_ids, cell_ids].add(increment)
        current = flat_temp.reshape(slab_shape)
    return current.reshape(initial_field.shape), interface
```

```python
import functools

import jax
import jax.numpy as jnp
from jax import lax
from jax.experimental import pallas as pl
from jax.experimental.pallas import tpu as pltpu
from jax.sharding import PartitionSpec as P

STEPS = 4
COUPLE = 4
ROWS = 128
HALO = 4
WIDE = 12
F32 = jnp.float32
BF16 = jnp.bfloat16
VMEM = pltpu.VMEM
SMEM = pltpu.SMEM


def iota(shape, dim):
    return lax.broadcasted_iota(jnp.int32, shape, dim)


def in_plane(x):
    return (
        pltpu.roll(x, 1, 0)
        + pltpu.roll(x, ROWS - 1, 0)
        + pltpu.roll(x, 1, 1)
        + pltpu.roll(x, 127, 1)
    )


def split(x):
    high = x.astype(BF16)
    return high, (x - high.astype(F32)).astype(BF16)


def run_steps(cur, nxt, coef, gas):
    bufs = (cur, nxt)
    for step in range(STEPS):
        src, dst = bufs[step % 2], bufs[(step + 1) % 2]

        def body(p, carry, src=src, dst=dst):
            x = src[p]
            down = src[p - 1]
            lap = src[p + 1] + down + in_plane(x) - 6.0 * x
            heat = gas * coef[2, p - 1]
            dst[p] = (
                x
                + coef[0, p - 1] * lap
                - gas * coef[1, p - 1] * (x - down)
                + heat * (0.5 + 0.5 * jnp.tanh(x))
            )
            return carry

        lax.fori_loop(step + 1, WIDE - 1 - step, body, 0)


def pick_nodes(tables, surf, count):
    lanes = [jnp.broadcast_to(surf[g : g + 1] & 127, (8, 128)) for g in range(4)]
    rows = [jnp.broadcast_to(surf[g : g + 1] >> 7, (8, 128)) - iota((8, 128), 0) for g in range(4)]

    def body(v, acc):
        out = []
        for t, table in enumerate(tables):
            tile = table(v)
            for g in range(4):
                got = jnp.take_along_axis(tile, lanes[g], axis=1, mode="promise_in_bounds")
                out.append(jnp.where(rows[g] == 8 * v, got, acc[4 * t + g]))
        return tuple(out)

    start = tuple(jnp.zeros((8, 128), F32) for _ in range(4 * len(tables)))
    acc = lax.fori_loop(0, count, body, start)
    return [
        jnp.concatenate([jnp.sum(acc[4 * t + g], axis=0, keepdims=True) for g in range(4)], axis=0)
        for t in range(len(tables))
    ]


def scatter_block(surf, inc):
    left, right = [], []
    for g in range(4):
        lane = surf[g : g + 1] & 127
        row = surf[g : g + 1] >> 7
        left.append(jnp.where(iota((256, 128), 0) == row, 1.0, 0.0).astype(BF16))
        hit = iota((128, 128), 0) == lane
        high = jnp.where(hit, inc[g : g + 1], 0.0)
        top = high.astype(BF16)
        low = (high - top.astype(F32)).astype(BF16)
        right.append(jnp.concatenate([top, low], axis=0))
    out = lax.dot_general(
        jnp.concatenate(left, axis=1),
        jnp.concatenate(right, axis=1),
        (((1,), (1,)), ((), ())),
        preferred_element_type=F32,
    )
    return out[:, :128] + out[:, 128:]


def finish(ints, cur, coef, surf_ref, flux, keep, export):
    core = ints[0]
    for p in range(4):
        keep[pl.ds(p * ROWS, ROWS), :] = cur[HALO + p]
    for p in range(2):
        x = cur[HALO + 2 * core + p]
        flux[pl.ds(p * ROWS, ROWS), :] = coef[0, HALO - 1 + 2 * core + p] * (4.0 * x - in_plane(x))

    def plane_tile(first):
        def tile(v):
            return cur[first + v // 16, pl.ds(pl.multiple_of((v % 16) * 8, 8), 8), :]

        return tile

    def flux_tile(v):
        return flux[pl.ds(pl.multiple_of(v * 8, 8), 8), :]

    own, own_flux = pick_nodes(
        [plane_tile(HALO + 2 * core), flux_tile], surf_ref[pl.ds(2 + core, 1)][0], 32
    )
    (mate,) = pick_nodes([plane_tile(HALO + 2 - 2 * core)], surf_ref[pl.ds(3 - core, 1)][0], 32)
    is_first = core == 0
    keep[pl.ds(4 * ROWS, 8), :] = jnp.concatenate(
        [jnp.where(is_first, own, mate), jnp.where(is_first, mate, own)], axis=0
    )
    block = jnp.concatenate([own, own_flux], axis=0)
    export[...] = jnp.broadcast_to(block[None], export.shape)


def first_kernel(ints, flts, own, mate, left, left_mate, right, right_mate,
                 keep, export, coef, surf, cur, nxt, flux):
    core = ints[0]
    other = 1 - core
    for base, mine, its in ((0, left, left_mate), (4, own, mate), (8, right, right_mate)):
        for p in range(2):
            cur[base + 2 * core + p] = mine[pl.ds(p * ROWS, ROWS), :]
            cur[base + 2 * other + p] = its[pl.ds(p * ROWS, ROWS), :]
        tail = mine[pl.ds(1024, 8), :].astype(jnp.int32)
        tail_mate = its[pl.ds(1024, 8), :].astype(jnp.int32)
        surf[pl.ds(base // 2 + core, 1)] = tail[:4][None]
        surf[pl.ds(base // 2 + other, 1)] = tail_mate[:4][None]
    for which in range(3):
        def rows(ref, p, which=which):
            return ref[pl.ds(256 * (which + 1) + p * ROWS, ROWS), :]

        for p in range(2):
            coef[which, 3 + 2 * core + p] = rows(own, p)
            coef[which, 3 + 2 * other + p] = rows(mate, p)
        coef[which, 0] = jnp.where(core == 0, rows(left, 1), rows(left_mate, 1))
        coef[which, 1] = jnp.where(core == 0, rows(left_mate, 0), rows(left, 0))
        coef[which, 2] = jnp.where(core == 0, rows(left_mate, 1), rows(left, 1))
        coef[which, 7] = jnp.where(core == 0, rows(right, 0), rows(right_mate, 0))
        coef[which, 8] = jnp.where(core == 0, rows(right, 1), rows(right_mate, 1))
        coef[which, 9] = jnp.where(core == 0, rows(right_mate, 0), rows(right, 0))
    run_steps(cur, nxt, coef, flts[2])
    finish(ints, cur, coef, surf, flux, keep, export)


def middle_kernel(ints, flts, parts, own, left, right, coef, surf, keep, export, cur, nxt, flux):
    total = lax.fori_loop(1, parts.shape[0], lambda i, acc: acc + parts[i], parts[0])
    for side, ref in enumerate((left, own, right)):
        temps = ref[pl.ds(4 * ROWS, 8), :]
        inc = total[8 * side : 8 * side + 8] - flts[0] * temps
        for half in range(2):
            block = 2 * side + half
            add = scatter_block(surf[block], inc[4 * half : 4 * half + 4])
            for p in range(2):
                row = (2 * half + p) * ROWS
                cur[2 * block + p] = ref[pl.ds(row, ROWS), :] + add[p * ROWS : (p + 1) * ROWS]
    run_steps(cur, nxt, coef, flts[2])
    finish(ints, cur, coef, surf, flux, keep, export)


def last_kernel(ints, flts, parts, own, surf, field, interface):
    core = ints[0]
    total = lax.fori_loop(1, parts.shape[0], lambda i, acc: acc + parts[i], parts[0])
    interface[...] = total
    temps = own[pl.ds(4 * ROWS, 8), :]
    temps = jnp.where(core == 0, temps[:4], temps[4:])
    inc = flts[0] * (total[:4] - temps) + flts[1] * total[4:]
    add = scatter_block(surf[pl.ds(2 + core, 1)][0], inc)
    start = pl.multiple_of(core * 2 * ROWS, 2 * ROWS)
    field[...] = own[pl.ds(start, 2 * ROWS), :] + add


def patch_kernel(ints, flts, source, local, targets, maps, out, *, final):
    slots = local.shape[0]
    parts = 2 if final else 1
    lanes = [local[pl.ds(8 * w, 8), :] & 127 for w in range(slots // 8)]
    rows = [local[pl.ds(8 * w, 8), :] >> 7 for w in range(slots // 8)]
    vals = [[jnp.zeros((8, 128), F32) for _ in rows] for _ in range(parts)]
    for i in range(3):
        tile = source[ints[3 + i]]
        tables = [tile[:4], tile[4:]] if final else [flts[0] * tile[:4] + flts[1] * tile[4:]]
        for q, table in enumerate(tables):
            for j in range(4):
                line = jnp.broadcast_to(table[j : j + 1], (8, 128))
                for w in range(slots // 8):
                    got = jnp.take_along_axis(line, lanes[w], axis=1, mode="promise_in_bounds")
                    vals[q][w] = jnp.where(rows[w] == 4 * i + j, got, vals[q][w])
    live = ints[1]
    columns = []
    for q in range(parts):
        held = [jnp.where(iota((8, 128), 0) + 8 * w < live, vals[q][w], 0.0) for w in range(slots // 8)]
        full = jnp.concatenate(held + [jnp.zeros((128 - slots, 128), F32)], axis=0)
        columns.append(full.T)
    left, right = [], [[] for _ in range(parts)]
    for s in range(slots):
        aim = targets[s : s + 1, :]
        left.append(jnp.where(iota((128, 128), 0) == aim >> 7, 1.0, 0.0).astype(BF16))
        hit = iota((128, 128), 0) == (aim & 127)
        table = maps[s]
        for q in range(parts):
            value = jnp.sum(table * columns[q][:, s : s + 1], axis=0, keepdims=True)
            top = value.astype(BF16).astype(F32)
            right[q].append(
                jnp.concatenate(
                    [jnp.where(hit, top, 0.0).astype(BF16), jnp.where(hit, value - top, 0.0).astype(BF16)],
                    axis=0,
                )
            )
    lhs = jnp.concatenate(left, axis=1)
    sums = []
    for q in range(parts):
        both = lax.dot_general(
            lhs, jnp.concatenate(right[q], axis=1), (((1,), (1,)), ((), ())), preferred_element_type=F32
        )
        sums.append(both[:, :128] + both[:, 128:])
    chips = out.shape[0] // 2
    for c in range(chips):
        if final:
            for k in range(2):
                r = 2 * c + k
                out[r] = jnp.concatenate([s[4 * r : 4 * r + 4] for s in sums], axis=0)
        else:
            for side in range(3):
                n = c + side - 1
                piece = sums[0][8 * n : 8 * n + 8] if 0 <= n < chips else jnp.zeros((8, 128), F32)
                for k in range(2):
                    out[2 * c + k, pl.ds(8 * side, 8), :] = piece


def call(kernel, n_in, outs, scratch=()):
    specs = [pl.BlockSpec(memory_space=SMEM)] * 2 + [pl.BlockSpec(memory_space=VMEM)] * (n_in - 2)
    return pl.pallas_call(
        kernel,
        out_shape=[jax.ShapeDtypeStruct(s, d) for s, d in outs],
        in_specs=specs,
        out_specs=[pl.BlockSpec(memory_space=VMEM)] * len(outs),
        scratch_shapes=[pltpu.VMEM(s, F32) for s in scratch],
        compiler_params=pltpu.CompilerParams(vmem_limit_bytes=40 * 1024 * 1024),
    )


def local(
    initial_field,
    conduct,
    velocity,
    heat_release,
    group_kind,
    partner,
    surface_cell,
    patch_count,
    patch_centres,
    patch_targets,
    patch_maps,
):
    subs = lax.axis_size("sub")
    groups = lax.axis_size("grp")
    me = lax.axis_index("sub")
    group = lax.axis_index("grp")
    nodes = surface_cell.shape[1] * subs
    block = surface_cell.shape[1]
    slots = patch_maps.shape[1]
    kind = group_kind[group]
    gain_temp = jnp.where(kind == 0, 0.5, 0.25).astype(F32)
    gain_flux = jnp.where(kind == 0, -0.25, 0.25).astype(F32)
    gas = (kind == 0).astype(F32)
    flts = jnp.stack([gain_temp, gain_flux, gas])

    rows = 2 * ROWS
    surf_rows = surface_cell.reshape(block // 128, 128).astype(F32)
    payload = jnp.concatenate(
        [a.reshape(rows, 128) for a in (initial_field, conduct, velocity, heat_release)]
        + [surf_rows, surf_rows],
        axis=0,
    )
    up = [(i, i + 2) for i in range(subs - 2)]
    down = [(i + 2, i) for i in range(subs - 2)]
    swap = [(i, i ^ 1) for i in range(subs)]
    left = lax.ppermute(payload, "sub", up)
    right = lax.ppermute(payload, "sub", down)
    mate = lax.ppermute(payload, "sub", swap)
    left_mate = lax.ppermute(left, "sub", swap)
    right_mate = lax.ppermute(right, "sub", swap)

    centres = patch_centres[0]
    targets = patch_targets[0]
    live = patch_count[0, me]
    anchor = centres[0, 0]
    apart = ((centres - anchor + nodes // 2) & (nodes - 1)) - nodes // 2
    apart = jnp.where(jnp.arange(slots)[:, None] < live, apart, 0)
    first = ((anchor + jnp.min(apart)) & (nodes - 1)) // block
    place = (centres - first * block) & (nodes - 1)
    base = partner[group] * subs
    ints = jnp.stack(
        [me & 1, live, group] + [base + ((first + i) & (subs - 1)) for i in range(3)]
    ).astype(jnp.int32)
    maps = jnp.swapaxes(patch_maps[0], 1, 2)

    keep_shape = ((4 * ROWS + 8, 128), F32)
    send_shape = ((groups * subs, 8, 128), F32)
    work = [(WIDE, ROWS, 128), (WIDE, ROWS, 128), (2 * ROWS, 128)]
    keep, send, coef, surf = call(
        first_kernel,
        8,
        [keep_shape, send_shape, ((3, WIDE - 2, ROWS, 128), F32), ((6, 4, 128), jnp.int32)],
        work,
    )(ints, flts, payload, mate, left, left_mate, right, right_mate)
    for iteration in range(COUPLE):
        final = iteration == COUPLE - 1
        if not final:
            left = lax.ppermute(keep, "sub", up)
            right = lax.ppermute(keep, "sub", down)
        source = lax.all_to_all(send, ("grp", "sub"), 0, 0, tiled=True)
        (parts,) = call(
            functools.partial(patch_kernel, final=final), 6, [((subs, 8 if final else 24, 128), F32)]
        )(ints, flts, source, place, targets, maps)
        parts = lax.all_to_all(parts, "sub", 0, 0, tiled=True)
        if final:
            field, interface = call(last_kernel, 5, [((2 * ROWS, 128), F32), ((8, 128), F32)])(
                ints, flts, parts, keep, surf
            )
        else:
            keep, send = call(middle_kernel, 8, [keep_shape, send_shape], work)(
                ints, flts, parts, keep, left, right, coef, surf
            )
    return field.reshape(initial_field.shape), interface.reshape(1, 2, block)


def solution(mesh):
    placed = (
        P("grp", "sub", None),
        P("grp", "sub", None),
        P("grp", "sub", None),
        P("grp", "sub", None),
        P(),
        P(),
        P("grp", "sub"),
        P("grp", None),
        P("grp", "sub", None),
        P("grp", "sub", None),
        P("grp", "sub", None, None),
    )
    return jax.shard_map(
        local,
        mesh=mesh,
        in_specs=placed,
        out_specs=(P("grp", "sub", None), P("grp", None, "sub")),
        check_vma=False,
    )
```

```python
import functools

import jax
import jax.numpy as jnp
from jax import lax
from jax.experimental import pallas as pl
from jax.experimental.pallas import tpu as pltpu
from jax.sharding import PartitionSpec as P

STEPS = 4
COUPLE = 4
ROWS = 128
HALO = 4
WIDE = 12
F32 = jnp.float32
BF16 = jnp.bfloat16
VMEM = pltpu.VMEM
SMEM = pltpu.SMEM


def iota(shape, dim):
    return lax.broadcasted_iota(jnp.int32, shape, dim)


def in_plane(x):
    return (
        pltpu.roll(x, 1, 0)
        + pltpu.roll(x, ROWS - 1, 0)
        + pltpu.roll(x, 1, 1)
        + pltpu.roll(x, 127, 1)
    )


def run_steps(cur, nxt, coef):
    bufs = (cur, nxt)
    for step in range(STEPS):
        src, dst = bufs[step % 2], bufs[(step + 1) % 2]

        def body(p, carry, src=src, dst=dst):
            x = src[p]
            dst[p] = (
                x
                + coef[0, p - 1] * (src[p + 1] + in_plane(x) - 5.0 * x)
                + coef[1, p - 1] * (src[p - 1] - x)
                + coef[2, p - 1] * (1.0 + jnp.tanh(x))
            )
            return carry

        lax.fori_loop(step + 1, WIDE - 1 - step, body, 0, unroll=2)


def pick_nodes(jobs):
    keys = []
    for _, surf in jobs:
        lanes = [jnp.broadcast_to(surf[g : g + 1] & 127, (8, 128)) for g in range(4)]
        rows = [jnp.broadcast_to(surf[g : g + 1] >> 7, (8, 128)) - iota((8, 128), 0) for g in range(4)]
        keys.append((lanes, rows))

    def body(v, acc):
        out = []
        for (tables, _), (lanes, rows) in zip(jobs, keys):
            hits = [rows[g] == 8 * v for g in range(4)]
            for table in tables:
                tile = table(v)
                for g in range(4):
                    got = jnp.take_along_axis(tile, lanes[g], axis=1, mode="promise_in_bounds")
                    out.append(jnp.where(hits[g], got, acc[len(out)]))
        return tuple(out)

    total = sum(len(tables) for tables, _ in jobs)
    acc = lax.fori_loop(0, 32, body, tuple(jnp.zeros((8, 128), F32) for _ in range(4 * total)), unroll=8)
    return [
        jnp.concatenate([jnp.sum(acc[4 * t + g], axis=0, keepdims=True) for g in range(4)], axis=0)
        for t in range(total)
    ]


def scatter_block(surf, inc):
    left, right = [], []
    for g in range(4):
        lane = surf[g : g + 1] & 127
        row = surf[g : g + 1] >> 7
        left.append(jnp.where(iota((256, 128), 0) == row, 1.0, 0.0).astype(BF16))
        hit = iota((128, 128), 0) == lane
        value = inc[g : g + 1]
        top = value.astype(BF16).astype(F32)
        right.append(
            jnp.concatenate(
                [jnp.where(hit, top, 0.0).astype(BF16), jnp.where(hit, value - top, 0.0).astype(BF16)], axis=0
            )
        )
    out = lax.dot_general(
        jnp.concatenate(left, axis=1),
        jnp.concatenate(right, axis=1),
        (((1,), (1,)), ((), ())),
        preferred_element_type=F32,
    )
    return out[:, :128] + out[:, 128:]


def finish(ints, flts, cur, coef, surf_ref, flux, keep, export, full):
    core = ints[0]
    for p in range(4):
        keep[pl.ds(p * ROWS, ROWS), :] = cur[HALO + p]
    for p in range(2):
        x = cur[HALO + 2 * core + p]
        flux[pl.ds(p * ROWS, ROWS), :] = coef[0, HALO - 1 + 2 * core + p] * (4.0 * x - in_plane(x))

    def plane_tile(first):
        def tile(v):
            return cur[first + v // 16, pl.ds(pl.multiple_of((v % 16) * 8, 8), 8), :]

        return tile

    def flux_tile(v):
        return flux[pl.ds(pl.multiple_of(v * 8, 8), 8), :]

    own, own_flux, mate = pick_nodes(
        [
            ([plane_tile(HALO + 2 * core), flux_tile], surf_ref[pl.ds(2 + core, 1)][0]),
            ([plane_tile(HALO + 2 - 2 * core)], surf_ref[pl.ds(3 - core, 1)][0]),
        ]
    )
    is_first = core == 0
    keep[pl.ds(4 * ROWS, 8), :] = jnp.concatenate(
        [jnp.where(is_first, own, mate), jnp.where(is_first, mate, own)], axis=0
    )
    if full:
        block = jnp.concatenate([own, own_flux], axis=0)
    else:
        block = flts[3] * own + flts[4] * own_flux
    export[...] = jnp.broadcast_to(block[None], export.shape)


def pack_kernel(field, conduct, velocity, heat, surface, payload):
    for i, ref in enumerate((field, conduct, velocity, heat)):
        payload[pl.ds(256 * i, 256), :] = ref[...].reshape(2 * ROWS, 128)
    cells = surface[...].reshape(4, 128).astype(F32)
    payload[pl.ds(1024, 8), :] = jnp.concatenate([cells, cells], axis=0)


def prepare_kernel(kinds, partners, counts, centres, maps, ints, flts, place, turned):
    group = lax.axis_index("grp")
    me = lax.axis_index("sub")
    subs = counts.shape[1]
    nodes = subs * 512
    live = counts[0, me]
    kind = kinds[group]
    at = centres[...]
    anchor = at[0:1, 0:1]
    apart = ((at - anchor + nodes // 2) & (nodes - 1)) - nodes // 2
    apart = jnp.where(iota(at.shape, 0) < live, apart, 0)
    lowest = jnp.min(apart.astype(F32)).astype(jnp.int32)
    start = (jnp.max(anchor.astype(F32)).astype(jnp.int32) + lowest) & (nodes - 1)
    first = start >> 9
    place[...] = (at - first * 512) & (nodes - 1)
    ints[0] = me & 1
    ints[1] = live
    ints[2] = kind
    for i in range(3):
        ints[3 + i] = partners[group] * subs + ((first + i) & (subs - 1))
    is_gas = kind == 0
    flts[0] = jnp.where(is_gas, 0.5, 0.25)
    flts[1] = jnp.where(is_gas, -0.25, 0.25)
    flts[2] = jnp.where(is_gas, 1.0, 0.0)
    flts[3] = jnp.where(is_gas, 0.25, 0.5)
    flts[4] = jnp.where(is_gas, 0.25, -0.25)
    for s in range(maps.shape[0]):
        turned[s] = maps[s].T


def first_kernel(ints, flts, own, mate, left, left_mate, right, right_mate,
                 keep, export, saved, surf, cur, nxt, flux, coef, sem):
    core = ints[0]
    other = 1 - core
    for base, mine, its in ((0, left, left_mate), (4, own, mate), (8, right, right_mate)):
        for p in range(2):
            cur[base + 2 * core + p] = mine[pl.ds(p * ROWS, ROWS), :]
            cur[base + 2 * other + p] = its[pl.ds(p * ROWS, ROWS), :]
        tail = mine[pl.ds(1024, 8), :].astype(jnp.int32)
        tail_mate = its[pl.ds(1024, 8), :].astype(jnp.int32)
        surf[pl.ds(base // 2 + core, 1)] = tail[:4][None]
        surf[pl.ds(base // 2 + other, 1)] = tail_mate[:4][None]
    gas = flts[2]

    def store(p, ref, half):
        got = [ref[pl.ds(256 * (w + 1) + half * ROWS, ROWS), :] for w in range(3)]
        coef[0, p] = got[0]
        coef[1, p] = got[0] + gas * got[1]
        coef[2, p] = (0.5 * gas) * got[2]

    for half in range(2):
        store(3 + 2 * core + half, own, half)
        store(3 + 2 * other + half, mate, half)

    @pl.when(core == 0)
    def _():
        store(0, left, 1)
        store(1, left_mate, 0)
        store(2, left_mate, 1)
        store(7, right, 0)
        store(8, right, 1)
        store(9, right_mate, 0)

    @pl.when(core == 1)
    def _():
        store(0, left_mate, 1)
        store(1, left, 0)
        store(2, left, 1)
        store(7, right_mate, 0)
        store(8, right_mate, 1)
        store(9, right, 0)

    copy = pltpu.make_async_copy(coef, saved, sem)
    copy.start()
    run_steps(cur, nxt, coef)
    finish(ints, flts, cur, coef, surf, flux, keep, export, False)
    copy.wait()


def middle_kernel(ints, flts, parts, own, left, right, surf, saved, keep, export,
                  cur, nxt, flux, coef, sem, *, full):
    copy = pltpu.make_async_copy(saved, coef, sem)
    copy.start()
    total = sum_parts(parts)
    for side, ref in enumerate((left, own, right)):
        temps = ref[pl.ds(4 * ROWS, 8), :]
        inc = total[8 * side : 8 * side + 8] - flts[0] * temps
        for half in range(2):
            block = 2 * side + half
            add = scatter_block(surf[block], inc[4 * half : 4 * half + 4])
            for p in range(2):
                row = (2 * half + p) * ROWS
                cur[2 * block + p] = ref[pl.ds(row, ROWS), :] + add[p * ROWS : (p + 1) * ROWS]
    copy.wait()
    run_steps(cur, nxt, coef)
    finish(ints, flts, cur, coef, surf, flux, keep, export, full)


def sum_parts(parts):
    lanes = [parts[i] for i in range(4)]
    for i in range(4, parts.shape[0]):
        lanes[i % 4] = lanes[i % 4] + parts[i]
    return (lanes[0] + lanes[1]) + (lanes[2] + lanes[3])


def last_kernel(ints, flts, parts, own, surf, field, interface):
    core = ints[0]
    total = sum_parts(parts)
    interface[...] = total.reshape(2, 512)
    temps = own[pl.ds(4 * ROWS, 8), :]
    temps = jnp.where(core == 0, temps[:4], temps[4:])
    inc = flts[0] * (total[:4] - temps) + flts[1] * total[4:]
    add = scatter_block(surf[pl.ds(2 + core, 1)][0], inc)
    start = pl.multiple_of(core * 2 * ROWS, 2 * ROWS)
    field[...] = (own[pl.ds(start, 2 * ROWS), :] + add).reshape(2, 128 * ROWS)


def patch_kernel(ints, flts, source, place, targets, turned, out, maps, sem, *, final):
    slots = place.shape[0]
    copy = pltpu.make_async_copy(turned, maps, sem)
    copy.start()
    parts = 2 if final else 1
    lanes = [place[pl.ds(8 * w, 8), :] & 127 for w in range(slots // 8)]
    rows = [place[pl.ds(8 * w, 8), :] >> 7 for w in range(slots // 8)]
    vals = [[jnp.zeros((8, 128), F32) for _ in rows] for _ in range(parts)]
    for i in range(3):
        tile = source[ints[3 + i]]
        for q in range(parts):
            for j in range(4):
                line = jnp.broadcast_to(tile[4 * q + j : 4 * q + j + 1], (8, 128))
                for w in range(slots // 8):
                    got = jnp.take_along_axis(line, lanes[w], axis=1, mode="promise_in_bounds")
                    vals[q][w] = jnp.where(rows[w] == 4 * i + j, got, vals[q][w])
    live = ints[1]
    columns = []
    for q in range(parts):
        held = [jnp.where(iota((8, 128), 0) + 8 * w < live, vals[q][w], 0.0) for w in range(slots // 8)]
        full = jnp.concatenate(held + [jnp.zeros((128 - slots, 128), F32)], axis=0)
        columns.append(full.T)
    copy.wait()
    left, right = [], [[] for _ in range(parts)]
    for s in range(slots):
        aim = targets[s : s + 1, :]
        left.append(jnp.where(iota((128, 128), 0) == aim >> 7, 1.0, 0.0).astype(BF16))
        hit = iota((128, 128), 0) == (aim & 127)
        table = maps[s]
        for q in range(parts):
            value = jnp.sum(table * columns[q][:, s : s + 1], axis=0, keepdims=True)
            top = value.astype(BF16).astype(F32)
            right[q].append(
                jnp.concatenate(
                    [jnp.where(hit, top, 0.0).astype(BF16), jnp.where(hit, value - top, 0.0).astype(BF16)],
                    axis=0,
                )
            )
    lhs = jnp.concatenate(left, axis=1)
    sums = []
    for q in range(parts):
        both = lax.dot_general(
            lhs, jnp.concatenate(right[q], axis=1), (((1,), (1,)), ((), ())), preferred_element_type=F32
        )
        sums.append(both[:, :128] + both[:, 128:])
    chips = out.shape[0] // 2
    for c in range(chips):
        if final:
            for k in range(2):
                r = 2 * c + k
                out[r] = jnp.concatenate([s[4 * r : 4 * r + 4] for s in sums], axis=0)
        else:
            for side in range(3):
                n = c + side - 1
                piece = sums[0][8 * n : 8 * n + 8] if 0 <= n < chips else jnp.zeros((8, 128), F32)
                for k in range(2):
                    out[2 * c + k, pl.ds(8 * side, 8), :] = piece


def call(kernel, ins, outs, scratch=()):
    where = {"s": SMEM, "v": VMEM, "h": pl.ANY}
    return pl.pallas_call(
        kernel,
        out_shape=[jax.ShapeDtypeStruct(s, d) for s, d, _ in outs],
        in_specs=[pl.BlockSpec(memory_space=where[i]) for i in ins],
        out_specs=[pl.BlockSpec(memory_space=where[o]) for _, _, o in outs],
        scratch_shapes=[pltpu.VMEM(s, F32) if s else pltpu.SemaphoreType.DMA for s in scratch],
        compiler_params=pltpu.CompilerParams(vmem_limit_bytes=16 * 1024 * 1024),
    )


def local(
    initial_field,
    conduct,
    velocity,
    heat_release,
    group_kind,
    partner,
    surface_cell,
    patch_count,
    patch_centres,
    patch_targets,
    patch_maps,
):
    subs = lax.axis_size("sub")
    groups = lax.axis_size("grp")
    block = surface_cell.shape[1]
    slots = patch_maps.shape[1]
    planes, cells = initial_field.shape[1:]

    (payload,) = call(pack_kernel, "vvvvv", [((1032, 128), F32, "v")])(
        *(a.reshape(planes, cells) for a in (initial_field, conduct, velocity, heat_release)),
        surface_cell,
    )
    up = [(i, i + 2) for i in range(subs - 2)]
    down = [(i + 2, i) for i in range(subs - 2)]
    swap = [(i, i ^ 1) for i in range(subs)]
    left = lax.ppermute(payload, "sub", up)
    right = lax.ppermute(payload, "sub", down)
    mate = lax.ppermute(payload, "sub", swap)
    ints, flts, place, turned = call(
        prepare_kernel,
        "sssvv",
        [
            ((6,), jnp.int32, "s"),
            ((5,), F32, "s"),
            ((slots, 128), jnp.int32, "v"),
            ((slots, 128, 128), F32, "v"),
        ],
    )(group_kind, partner, patch_count, patch_centres[0], patch_maps[0])
    targets = patch_targets[0]
    left_mate = lax.ppermute(left, "sub", swap)
    right_mate = lax.ppermute(right, "sub", swap)

    keep_out = ((4 * ROWS + 8, 128), F32, "v")
    half_out = ((groups * subs, 4, 128), F32, "v")
    full_out = ((groups * subs, 8, 128), F32, "v")
    coef_shape = (3, WIDE - 2, ROWS, 128)
    work = [(WIDE, ROWS, 128), (WIDE, ROWS, 128), (2 * ROWS, 128), coef_shape, None]
    keep, send, coef, surf = call(
        first_kernel,
        "ssvvvvvv",
        [keep_out, half_out, (coef_shape, F32, "h"), ((6, 4, 128), jnp.int32, "v")],
        work,
    )(ints, flts, payload, mate, left, left_mate, right, right_mate)
    for iteration in range(COUPLE):
        final = iteration == COUPLE - 1
        if not final:
            left = lax.ppermute(keep, "sub", up)
            right = lax.ppermute(keep, "sub", down)
        source = lax.all_to_all(send, ("grp", "sub"), 0, 0, tiled=True)
        (parts,) = call(
            functools.partial(patch_kernel, final=final),
            "ssvvvh",
            [((subs, 8 if final else 24, 128), F32, "v")],
            [(slots, 128, 128), None],
        )(ints, flts, source, place, targets, turned)
        parts = lax.all_to_all(parts, "sub", 0, 0, tiled=True)
        if final:
            field, interface = call(
                last_kernel, "ssvvv", [((planes, cells), F32, "v"), ((2, block), F32, "v")]
            )(ints, flts, parts, keep, surf)
        else:
            full = iteration == COUPLE - 2
            keep, send = call(
                functools.partial(middle_kernel, full=full),
                "ssvvvvvh",
                [keep_out, full_out if full else half_out],
                work,
            )(ints, flts, parts, keep, left, right, surf, coef)
    return field[None], interface[None]


def solution(mesh):
    placed = (
        P("grp", "sub", None),
        P("grp", "sub", None),
        P("grp", "sub", None),
        P("grp", "sub", None),
        P(),
        P(),
        P("grp", "sub"),
        P("grp", None),
        P("grp", "sub", None),
        P("grp", "sub", None),
        P("grp", "sub", None, None),
    )
    return jax.shard_map(
        local,
        mesh=mesh,
        in_specs=placed,
        out_specs=(P("grp", "sub", None), P("grp", None, "sub")),
        check_vma=False,
    )
```

```python
import functools

import jax
import jax.numpy as jnp
from jax import lax
from jax.experimental import pallas as pl
from jax.experimental.pallas import tpu as pltpu
from jax.sharding import PartitionSpec as P


STEPS = 4
COUPLE = 4
ROWS = 128
HALO = 4
WIDE = 12
F32 = jnp.float32
BF16 = jnp.bfloat16
VMEM = pltpu.VMEM
SMEM = pltpu.SMEM


def iota(shape, dim):
    return lax.broadcasted_iota(jnp.int32, shape, dim)


def in_plane(x):
    return (
        pltpu.roll(x, 1, 0)
        + pltpu.roll(x, ROWS - 1, 0)
        + pltpu.roll(x, 1, 1)
        + pltpu.roll(x, 127, 1)
    )


def run_steps(cur, nxt, coef):
    bufs = (cur, nxt)
    for step in range(STEPS):
        src, dst = bufs[step % 2], bufs[(step + 1) % 2]

        def body(p, carry, src=src, dst=dst):
            x = src[p]
            dst[p] = (
                x
                + coef[0, p - 1] * (src[p + 1] + in_plane(x) - 5.0 * x)
                + coef[1, p - 1] * (src[p - 1] - x)
                + coef[2, p - 1] * (1.0 + jnp.tanh(x))
            )
            return carry

        lax.fori_loop(step + 1, WIDE - 1 - step, body, 0, unroll=2)


def pick_nodes(jobs):
    keys = []
    for _, surf in jobs:
        lanes = [jnp.broadcast_to(surf[g : g + 1] & 127, (8, 128)) for g in range(4)]
        rows = [jnp.broadcast_to(surf[g : g + 1] >> 7, (8, 128)) - iota((8, 128), 0) for g in range(4)]
        keys.append((lanes, rows))

    def body(v, acc):
        out = []
        for (tables, _), (lanes, rows) in zip(jobs, keys):
            hits = [rows[g] == 8 * v for g in range(4)]
            for table in tables:
                tile = table(v)
                for g in range(4):
                    got = jnp.take_along_axis(tile, lanes[g], axis=1, mode="promise_in_bounds")
                    out.append(jnp.where(hits[g], got, acc[len(out)]))
        return tuple(out)

    total = sum(len(tables) for tables, _ in jobs)
    acc = lax.fori_loop(0, 32, body, tuple(jnp.zeros((8, 128), F32) for _ in range(4 * total)), unroll=8)
    return [
        jnp.concatenate([jnp.sum(acc[4 * t + g], axis=0, keepdims=True) for g in range(4)], axis=0)
        for t in range(total)
    ]


def scatter_block(surf, inc):
    left, right = [], []
    for g in range(4):
        lane = surf[g : g + 1] & 127
        row = surf[g : g + 1] >> 7
        left.append(jnp.where(iota((256, 128), 0) == row, 1.0, 0.0).astype(BF16))
        hit = iota((128, 128), 0) == lane
        value = inc[g : g + 1]
        top = value.astype(BF16).astype(F32)
        right.append(
            jnp.concatenate(
                [jnp.where(hit, top, 0.0).astype(BF16), jnp.where(hit, value - top, 0.0).astype(BF16)], axis=0
            )
        )
    out = lax.dot_general(
        jnp.concatenate(left, axis=1),
        jnp.concatenate(right, axis=1),
        (((1,), (1,)), ((), ())),
        preferred_element_type=F32,
    )
    return out[:, :128] + out[:, 128:]


def finish(ints, flts, cur, coef, surf_ref, flux, keep, export, full):
    core = ints[0]
    for p in range(4):
        keep[pl.ds(p * ROWS, ROWS), :] = cur[HALO + p]
    for p in range(2):
        x = cur[HALO + 2 * core + p]
        flux[pl.ds(p * ROWS, ROWS), :] = coef[0, HALO - 1 + 2 * core + p] * (4.0 * x - in_plane(x))

    def plane_tile(first):
        def tile(v):
            return cur[first + v // 16, pl.ds(pl.multiple_of((v % 16) * 8, 8), 8), :]

        return tile

    def flux_tile(v):
        return flux[pl.ds(pl.multiple_of(v * 8, 8), 8), :]

    own, own_flux, mate = pick_nodes(
        [
            ([plane_tile(HALO + 2 * core), flux_tile], surf_ref[pl.ds(2 + core, 1)][0]),
            ([plane_tile(HALO + 2 - 2 * core)], surf_ref[pl.ds(3 - core, 1)][0]),
        ]
    )
    is_first = core == 0
    keep[pl.ds(4 * ROWS, 8), :] = jnp.concatenate(
        [jnp.where(is_first, own, mate), jnp.where(is_first, mate, own)], axis=0
    )
    if full:
        block = jnp.concatenate([own, own_flux], axis=0)
    else:
        block = flts[3] * own + flts[4] * own_flux
    export[...] = jnp.broadcast_to(block[None], export.shape)


def pack_kernel(fields, surface, payload):
    for i in range(4):
        payload[pl.ds(256 * i, 256), :] = fields[i].reshape(2 * ROWS, 128)
    cells = surface[...].reshape(4, 128).astype(F32)
    payload[pl.ds(1024, 8), :] = jnp.concatenate([cells, cells], axis=0)


def prepare_kernel(kinds, partners, counts, centres, maps, ints, flts, place, turned):
    group = lax.axis_index("grp")
    me = lax.axis_index("sub")
    subs = counts.shape[1]
    nodes = subs * 512
    live = counts[0, me]
    kind = kinds[group]
    at = centres[...]
    anchor = at[0:1, 0:1]
    apart = ((at - anchor + nodes // 2) & (nodes - 1)) - nodes // 2
    apart = jnp.where(iota(at.shape, 0) < live, apart, 0)
    lowest = jnp.min(apart.astype(F32)).astype(jnp.int32)
    start = (jnp.max(anchor.astype(F32)).astype(jnp.int32) + lowest) & (nodes - 1)
    first = start >> 9
    place[...] = (at - first * 512) & (nodes - 1)
    ints[0] = me & 1
    ints[1] = live
    ints[2] = kind
    for i in range(3):
        ints[3 + i] = partners[group] * subs + ((first + i) & (subs - 1))
    is_gas = kind == 0
    flts[0] = jnp.where(is_gas, 0.5, 0.25)
    flts[1] = jnp.where(is_gas, -0.25, 0.25)
    flts[2] = jnp.where(is_gas, 1.0, 0.0)
    flts[3] = jnp.where(is_gas, 0.25, 0.5)
    flts[4] = jnp.where(is_gas, 0.25, -0.25)
    for s in range(maps.shape[0]):
        turned[s] = maps[s].T


def first_kernel(ints, flts, own, mate, left, left_mate, right, right_mate,
                 keep, export, coef, surf, cur, nxt, flux):
    core = ints[0]
    other = 1 - core
    for base, mine, its in ((0, left, left_mate), (4, own, mate), (8, right, right_mate)):
        for p in range(2):
            cur[base + 2 * core + p] = mine[pl.ds(p * ROWS, ROWS), :]
            cur[base + 2 * other + p] = its[pl.ds(p * ROWS, ROWS), :]
        tail = mine[pl.ds(1024, 8), :].astype(jnp.int32)
        tail_mate = its[pl.ds(1024, 8), :].astype(jnp.int32)
        surf[pl.ds(base // 2 + core, 1)] = tail[:4][None]
        surf[pl.ds(base // 2 + other, 1)] = tail_mate[:4][None]
    gas = flts[2]

    def store(p, ref, half):
        got = [ref[pl.ds(256 * (w + 1) + half * ROWS, ROWS), :] for w in range(3)]
        coef[0, p] = got[0]
        coef[1, p] = got[0] + gas * got[1]
        coef[2, p] = (0.5 * gas) * got[2]

    for half in range(2):
        store(3 + 2 * core + half, own, half)
        store(3 + 2 * other + half, mate, half)

    @pl.when(core == 0)
    def _():
        store(0, left, 1)
        store(1, left_mate, 0)
        store(2, left_mate, 1)
        store(7, right, 0)
        store(8, right, 1)
        store(9, right_mate, 0)

    @pl.when(core == 1)
    def _():
        store(0, left_mate, 1)
        store(1, left, 0)
        store(2, left, 1)
        store(7, right_mate, 0)
        store(8, right_mate, 1)
        store(9, right, 0)

    run_steps(cur, nxt, coef)
    finish(ints, flts, cur, coef, surf, flux, keep, export, False)


def middle_kernel(ints, flts, parts, own, beside, other, surf, coef, keep, export,
                  cur, nxt, flux, *, full):
    first = ints[0] == 0
    total = sum_parts(parts)

    def sides(start, size):
        near = beside[pl.ds(start, size), :]
        far = other[pl.ds(start, size), :]
        return jnp.where(first, near, far), own[pl.ds(start, size), :], jnp.where(first, far, near)

    temps = sides(4 * ROWS, 8)
    incs = [total[8 * side : 8 * side + 8] - flts[0] * temps[side] for side in range(3)]
    for half in range(2):
        planes = sides(2 * half * ROWS, 2 * ROWS)
        for side in range(3):
            block = 2 * side + half
            out = planes[side] + scatter_block(surf[block], incs[side][4 * half : 4 * half + 4])
            cur[2 * block] = out[:ROWS]
            cur[2 * block + 1] = out[ROWS:]
    run_steps(cur, nxt, coef)
    finish(ints, flts, cur, coef, surf, flux, keep, export, full)


def sum_parts(parts):
    lanes = [parts[i] for i in range(4)]
    for i in range(4, parts.shape[0]):
        lanes[i % 4] = lanes[i % 4] + parts[i]
    return (lanes[0] + lanes[1]) + (lanes[2] + lanes[3])


def last_kernel(ints, flts, parts, own, surf, field, interface):
    core = ints[0]
    total = sum_parts(parts)
    interface[...] = total.reshape(2, 512)
    temps = own[pl.ds(4 * ROWS, 8), :]
    temps = jnp.where(core == 0, temps[:4], temps[4:])
    inc = flts[0] * (total[:4] - temps) + flts[1] * total[4:]
    add = scatter_block(surf[pl.ds(2 + core, 1)][0], inc)
    start = pl.multiple_of(core * 2 * ROWS, 2 * ROWS)
    field[...] = (own[pl.ds(start, 2 * ROWS), :] + add).reshape(2, 128 * ROWS)


def patch_kernel(ints, flts, source, place, targets, maps, out, *, final):
    slots = place.shape[0]
    parts = 2 if final else 1
    lanes = [place[pl.ds(8 * w, 8), :] & 127 for w in range(slots // 8)]
    rows = [place[pl.ds(8 * w, 8), :] >> 7 for w in range(slots // 8)]
    vals = [[jnp.zeros((8, 128), F32) for _ in rows] for _ in range(parts)]
    for i in range(3):
        tile = source[ints[3 + i]]
        for q in range(parts):
            for j in range(4):
                line = jnp.broadcast_to(tile[4 * q + j : 4 * q + j + 1], (8, 128))
                for w in range(slots // 8):
                    got = jnp.take_along_axis(line, lanes[w], axis=1, mode="promise_in_bounds")
                    vals[q][w] = jnp.where(rows[w] == 4 * i + j, got, vals[q][w])
    live = ints[1]
    columns = []
    for q in range(parts):
        held = [jnp.where(iota((8, 128), 0) + 8 * w < live, vals[q][w], 0.0) for w in range(slots // 8)]
        full = jnp.concatenate(held + [jnp.zeros((128 - slots, 128), F32)], axis=0)
        columns.append(full.T)
    left, right = [], [[] for _ in range(parts)]
    for s in range(slots):
        aim = targets[s : s + 1, :]
        left.append(jnp.where(iota((128, 128), 0) == aim >> 7, 1.0, 0.0).astype(BF16))
        hit = iota((128, 128), 0) == (aim & 127)
        table = maps[s]
        for q in range(parts):
            value = jnp.sum(table * columns[q][:, s : s + 1], axis=0, keepdims=True)
            top = value.astype(BF16).astype(F32)
            right[q].append(
                jnp.concatenate(
                    [jnp.where(hit, top, 0.0).astype(BF16), jnp.where(hit, value - top, 0.0).astype(BF16)],
                    axis=0,
                )
            )
    lhs = jnp.concatenate(left, axis=1)
    sums = []
    for q in range(parts):
        both = lax.dot_general(
            lhs, jnp.concatenate(right[q], axis=1), (((1,), (1,)), ((), ())), preferred_element_type=F32
        )
        sums.append(both[:, :128] + both[:, 128:])
    chips = out.shape[0] // 2
    for c in range(chips):
        if final:
            for k in range(2):
                r = 2 * c + k
                out[r] = jnp.concatenate([s[4 * r : 4 * r + 4] for s in sums], axis=0)
        else:
            for side in range(3):
                n = c + side - 1
                piece = sums[0][8 * n : 8 * n + 8] if 0 <= n < chips else jnp.zeros((8, 128), F32)
                for k in range(2):
                    out[2 * c + k, pl.ds(8 * side, 8), :] = piece


def call(kernel, ins, outs, scratch=()):
    where = {"s": SMEM, "v": VMEM}
    return pl.pallas_call(
        kernel,
        out_shape=[jax.ShapeDtypeStruct(s, d) for s, d, _ in outs],
        in_specs=[pl.BlockSpec(memory_space=where[i]) for i in ins],
        out_specs=[pl.BlockSpec(memory_space=where[o]) for _, _, o in outs],
        scratch_shapes=[pltpu.VMEM(s, F32) for s in scratch],
        compiler_params=pltpu.CompilerParams(vmem_limit_bytes=16 * 1024 * 1024),
    )


def local(
    initial_field,
    conduct,
    velocity,
    heat_release,
    group_kind,
    partner,
    surface_cell,
    patch_count,
    patch_centres,
    patch_targets,
    patch_maps,
):
    subs = lax.axis_size("sub")
    groups = lax.axis_size("grp")
    block = surface_cell.shape[1]
    slots = patch_maps.shape[1]
    planes, cells = initial_field.shape[1:]

    fields = jnp.concatenate([initial_field, conduct, velocity, heat_release], axis=0)
    (payload,) = call(pack_kernel, "vv", [((1032, 128), F32, "v")])(fields, surface_cell)
    up = [(i, i + 2) for i in range(subs - 2)]
    down = [(i + 2, i) for i in range(subs - 2)]
    swap = [(i, i ^ 1) for i in range(subs)]
    cross = [(i, i + 1 if i % 2 else i - 1) for i in range(1, subs - 1)]
    left = lax.ppermute(payload, "sub", up)
    right = lax.ppermute(payload, "sub", down)
    mate = lax.ppermute(payload, "sub", swap)
    ints, flts, place, turned = call(
        prepare_kernel,
        "sssvv",
        [
            ((6,), jnp.int32, "s"),
            ((5,), F32, "s"),
            ((slots, 128), jnp.int32, "v"),
            ((slots, 128, 128), F32, "v"),
        ],
    )(group_kind, partner, patch_count, patch_centres[0], patch_maps[0])
    targets = patch_targets[0]
    left_mate = lax.ppermute(left, "sub", swap)
    right_mate = lax.ppermute(right, "sub", swap)

    keep_out = ((4 * ROWS + 8, 128), F32, "v")
    half_out = ((groups * subs, 4, 128), F32, "v")
    full_out = ((groups * subs, 8, 128), F32, "v")
    coef_shape = (3, WIDE - 2, ROWS, 128)
    work = [(WIDE, ROWS, 128), (WIDE, ROWS, 128), (2 * ROWS, 128)]
    keep, send, coef, surf = call(
        first_kernel,
        "ssvvvvvv",
        [keep_out, half_out, (coef_shape, F32, "v"), ((6, 4, 128), jnp.int32, "v")],
        work,
    )(ints, flts, payload, mate, left, left_mate, right, right_mate)
    for iteration in range(COUPLE):
        final = iteration == COUPLE - 1
        if not final:
            beside = lax.ppermute(keep, "sub", cross)
        source = lax.all_to_all(send, ("grp", "sub"), 0, 0, tiled=True)
        if not final:
            source, beside = lax.optimization_barrier((source, beside))
            other = lax.ppermute(beside, "sub", swap)
        (parts,) = call(
            functools.partial(patch_kernel, final=final),
            "ssvvvv",
            [((subs, 8 if final else 24, 128), F32, "v")],
        )(ints, flts, source, place, targets, turned)
        if not final:
            parts, other = lax.optimization_barrier((parts, other))
        parts = lax.all_to_all(parts, "sub", 0, 0, tiled=True)
        if final:
            field, interface = call(
                last_kernel, "ssvvv", [((planes, cells), F32, "v"), ((2, block), F32, "v")]
            )(ints, flts, parts, keep, surf)
        else:
            full = iteration == COUPLE - 2
            keep, send = call(
                functools.partial(middle_kernel, full=full),
                "ssvvvvvv",
                [keep_out, full_out if full else half_out],
                work,
            )(ints, flts, parts, keep, beside, other, surf, coef)
    return field[None], interface[None]


def solution(mesh):
    placed = (
        P("grp", "sub", None),
        P("grp", "sub", None),
        P("grp", "sub", None),
        P("grp", "sub", None),
        P(),
        P(),
        P("grp", "sub"),
        P("grp", None),
        P("grp", "sub", None),
        P("grp", "sub", None),
        P("grp", "sub", None, None),
    )
    return jax.shard_map(
        local,
        mesh=mesh,
        in_specs=placed,
        out_specs=(P("grp", "sub", None), P("grp", None, "sub")),
        check_vma=False,
    )
```

```python
import functools

import jax
import jax.numpy as jnp
from jax import lax
from jax.experimental import pallas as pl
from jax.experimental.pallas import tpu as pltpu
from jax.sharding import PartitionSpec as P


STEPS = 4
COUPLE = 4
ROWS = 128
HALO = 4
WIDE = 12
F32 = jnp.float32
BF16 = jnp.bfloat16
VMEM = pltpu.VMEM
SMEM = pltpu.SMEM


def iota(shape, dim):
    return lax.broadcasted_iota(jnp.int32, shape, dim)


def in_plane(x):
    return (
        pltpu.roll(x, 1, 0)
        + pltpu.roll(x, ROWS - 1, 0)
        + pltpu.roll(x, 1, 1)
        + pltpu.roll(x, 127, 1)
    )


def run_steps(cur, nxt, coef):
    bufs = (cur, nxt)
    for step in range(STEPS):
        src, dst = bufs[step % 2], bufs[(step + 1) % 2]

        def body(p, carry, src=src, dst=dst):
            x = src[p]
            dst[p] = (
                x
                + coef[0, p - 1] * (src[p + 1] + in_plane(x) - 5.0 * x)
                + coef[1, p - 1] * (src[p - 1] - x)
                + coef[2, p - 1] * (1.0 + jnp.tanh(x))
            )
            return carry

        lax.fori_loop(step + 1, WIDE - 1 - step, body, 0, unroll=2)


def pick_nodes(jobs):
    keys = []
    for _, surf in jobs:
        lanes = [jnp.broadcast_to(surf[g : g + 1] & 127, (8, 128)) for g in range(4)]
        rows = [jnp.broadcast_to(surf[g : g + 1] >> 7, (8, 128)) - iota((8, 128), 0) for g in range(4)]
        keys.append((lanes, rows))

    def body(v, acc):
        out = []
        for (tables, _), (lanes, rows) in zip(jobs, keys):
            hits = [rows[g] == 8 * v for g in range(4)]
            for table in tables:
                tile = table(v)
                for g in range(4):
                    got = jnp.take_along_axis(tile, lanes[g], axis=1, mode="promise_in_bounds")
                    out.append(jnp.where(hits[g], got, acc[len(out)]))
        return tuple(out)

    total = sum(len(tables) for tables, _ in jobs)
    acc = lax.fori_loop(0, 32, body, tuple(jnp.zeros((8, 128), F32) for _ in range(4 * total)), unroll=8)
    return [
        jnp.concatenate([jnp.sum(acc[4 * t + g], axis=0, keepdims=True) for g in range(4)], axis=0)
        for t in range(total)
    ]


def halves(x):
    high = x.astype(BF16)
    return high, (x - high.astype(F32)).astype(BF16)


def rows_at(index, count):
    return iota((count, 128), 0).astype(F32).astype(BF16) == index.astype(F32).astype(BF16)


def one_hot(index, count):
    return jnp.where(rows_at(index, count), jnp.bfloat16(1), jnp.bfloat16(0))


def spread(index, value):
    hit = rows_at(index, 128)
    return jnp.concatenate([jnp.where(hit, part, jnp.bfloat16(0)) for part in halves(value)], axis=0)


def product(left, right):
    out = lax.dot_general(
        jnp.concatenate(left, axis=1),
        jnp.concatenate(right, axis=1),
        (((1,), (1,)), ((), ())),
        preferred_element_type=F32,
    )
    return out[:, :128] + out[:, 128:]


def scatter_block(surf, inc):
    groups = [slice(g, g + 1) for g in range(4)]
    return product(
        [one_hot(surf[g] >> 7, 256) for g in groups], [spread(surf[g] & 127, inc[g]) for g in groups]
    )


def finish(flts, cur, coef, surf_ref, flux, keep, export, full):
    core = lax.axis_index("sub") & 1
    for p in range(4):
        keep[pl.ds(p * ROWS, ROWS), :] = cur[HALO + p]
    for p in range(2):
        x = cur[HALO + 2 * core + p]
        flux[pl.ds(p * ROWS, ROWS), :] = coef[0, HALO - 1 + 2 * core + p] * (4.0 * x - in_plane(x))

    def plane_tile(first):
        def tile(v):
            return cur[first + v // 16, pl.ds(pl.multiple_of((v % 16) * 8, 8), 8), :]

        return tile

    def flux_tile(v):
        return flux[pl.ds(pl.multiple_of(v * 8, 8), 8), :]

    own, own_flux, mate = pick_nodes(
        [
            ([plane_tile(HALO + 2 * core), flux_tile], surf_ref[pl.ds(2 + core, 1)][0]),
            ([plane_tile(HALO + 2 - 2 * core)], surf_ref[pl.ds(3 - core, 1)][0]),
        ]
    )
    is_first = core == 0
    keep[pl.ds(4 * ROWS, 8), :] = jnp.concatenate(
        [jnp.where(is_first, own, mate), jnp.where(is_first, mate, own)], axis=0
    )
    if full:
        block = jnp.concatenate([own, own_flux], axis=0)
    else:
        block = flts[3:4, :] * own + flts[4:5, :] * own_flux
    export[...] = jnp.broadcast_to(block[None], export.shape)


def pack_kernel(fields, surface, payload):
    for i in range(4):
        payload[pl.ds(256 * i, 256), :] = fields[i].reshape(2 * ROWS, 128)
    cells = surface[...].reshape(4, 128).astype(F32)
    payload[pl.ds(1024, 8), :] = jnp.concatenate([cells, cells], axis=0)


def prepare_kernel(kinds, partners, counts, centres, maps, ints, flts, place, turned):
    group = lax.axis_index("grp")
    me = lax.axis_index("sub")
    subs = counts.shape[1]
    nodes = subs * 512
    live = counts[0, me]
    kind = kinds[group]
    at = centres[...]
    anchor = at[0:1, 0:1]
    apart = ((at - anchor + nodes // 2) & (nodes - 1)) - nodes // 2
    apart = jnp.where(iota(at.shape, 0) < live, apart, 0)
    lowest = jnp.min(apart.astype(F32)).astype(jnp.int32)
    start = (jnp.max(anchor.astype(F32)).astype(jnp.int32) + lowest) & (nodes - 1)
    first = start >> 9
    place[...] = jnp.where(iota(at.shape, 0) < live, (at - first * 512) & (nodes - 1), -1)
    ints[...] = jnp.full(ints.shape, partners[group] * subs + first, jnp.int32)
    is_gas = kind == 0
    for row, (gas, solid) in enumerate(((0.5, 0.25), (-0.25, 0.25), (1.0, 0.0), (0.25, 0.5), (0.25, -0.25))):
        flts[pl.ds(row, 1), :] = jnp.full((1, 128), jnp.where(is_gas, gas, solid), F32)
    for s in range(maps.shape[0]):
        turned[s] = maps[s].T


def first_kernel(flts, own, mate, left, left_mate, right, right_mate,
                 keep, export, coef, surf, cur, nxt, flux):
    core = lax.axis_index("sub") & 1
    other = 1 - core
    for base, mine, its in ((0, left, left_mate), (4, own, mate), (8, right, right_mate)):
        for p in range(2):
            cur[base + 2 * core + p] = mine[pl.ds(p * ROWS, ROWS), :]
            cur[base + 2 * other + p] = its[pl.ds(p * ROWS, ROWS), :]
        tail = mine[pl.ds(1024, 8), :].astype(jnp.int32)
        tail_mate = its[pl.ds(1024, 8), :].astype(jnp.int32)
        surf[pl.ds(base // 2 + core, 1)] = tail[:4][None]
        surf[pl.ds(base // 2 + other, 1)] = tail_mate[:4][None]
    gas = flts[2:3, :]

    def store(p, ref, half):
        got = [ref[pl.ds(256 * (w + 1) + half * ROWS, ROWS), :] for w in range(3)]
        coef[0, p] = got[0]
        coef[1, p] = got[0] + gas * got[1]
        coef[2, p] = (0.5 * gas) * got[2]

    for half in range(2):
        store(3 + 2 * core + half, own, half)
        store(3 + 2 * other + half, mate, half)

    @pl.when(core == 0)
    def _():
        store(0, left, 1)
        store(1, left_mate, 0)
        store(2, left_mate, 1)
        store(7, right, 0)
        store(8, right, 1)
        store(9, right_mate, 0)

    @pl.when(core == 1)
    def _():
        store(0, left_mate, 1)
        store(1, left, 0)
        store(2, left, 1)
        store(7, right_mate, 0)
        store(8, right_mate, 1)
        store(9, right, 0)

    run_steps(cur, nxt, coef)
    finish(flts, cur, coef, surf, flux, keep, export, False)


def middle_kernel(flts, parts, own, beside, other, surf, coef, keep, export,
                  cur, nxt, flux, *, full):
    first = (lax.axis_index("sub") & 1) == 0
    total = sum_parts(parts)

    def sides(start, size):
        near = beside[pl.ds(start, size), :]
        far = other[pl.ds(start, size), :]
        return jnp.where(first, near, far), own[pl.ds(start, size), :], jnp.where(first, far, near)

    temps = sides(4 * ROWS, 8)
    incs = [total[8 * side : 8 * side + 8] - flts[0:1, :] * temps[side] for side in range(3)]
    for half in range(2):
        planes = sides(2 * half * ROWS, 2 * ROWS)
        for side in range(3):
            block = 2 * side + half
            out = planes[side] + scatter_block(surf[block], incs[side][4 * half : 4 * half + 4])
            cur[2 * block] = out[:ROWS]
            cur[2 * block + 1] = out[ROWS:]
    run_steps(cur, nxt, coef)
    finish(flts, cur, coef, surf, flux, keep, export, full)


def sum_parts(parts):
    lanes = [parts[i] for i in range(4)]
    for i in range(4, parts.shape[0]):
        lanes[i % 4] = lanes[i % 4] + parts[i]
    return (lanes[0] + lanes[1]) + (lanes[2] + lanes[3])


def last_kernel(flts, parts, own, surf, field, interface):
    core = lax.axis_index("sub") & 1
    total = sum_parts(parts)
    interface[...] = total.reshape(2, 512)
    temps = own[pl.ds(4 * ROWS, 8), :]
    temps = jnp.where(core == 0, temps[:4], temps[4:])
    inc = flts[0:1, :] * (total[:4] - temps) + flts[1:2, :] * total[4:]
    add = scatter_block(surf[pl.ds(2 + core, 1)][0], inc)
    start = pl.multiple_of(core * 2 * ROWS, 2 * ROWS)
    field[...] = (own[pl.ds(start, 2 * ROWS), :] + add).reshape(2, 128 * ROWS)


def patch_kernel(ints, source, place, targets, maps, out, *, final):
    slots = place.shape[0]
    subs = out.shape[0]
    parts = 2 if final else 1
    lanes = [place[pl.ds(8 * w, 8), :] & 127 for w in range(slots // 8)]
    rows = [place[pl.ds(8 * w, 8), :] >> 7 for w in range(slots // 8)]
    vals = [[jnp.zeros((8, 128), F32) for _ in rows] for _ in range(parts)]
    at = jnp.max(ints[0:1, :].astype(F32)).astype(jnp.int32)
    for i in range(3):
        tile = source[(at & -subs) + ((at + i) & (subs - 1))]
        for q in range(parts):
            for j in range(4):
                line = jnp.broadcast_to(tile[4 * q + j : 4 * q + j + 1], (8, 128))
                for w in range(slots // 8):
                    got = jnp.take_along_axis(line, lanes[w], axis=1, mode="promise_in_bounds")
                    vals[q][w] = jnp.where(rows[w] == 4 * i + j, got, vals[q][w])
    columns = []
    for q in range(parts):
        full = jnp.concatenate(vals[q] + [jnp.zeros((128 - slots, 128), F32)], axis=0)
        columns.append(full.T)
    left, right = [], [[] for _ in range(parts)]
    for s in range(slots):
        aim = targets[s : s + 1, :]
        left.append(one_hot(aim >> 7, 128))
        table = maps[s]
        for q in range(parts):
            value = jnp.sum(table * columns[q][:, s : s + 1], axis=0, keepdims=True)
            right[q].append(spread(aim & 127, value))
    sums = [product(left, right[q]) for q in range(parts)]
    chips = out.shape[0] // 2
    for c in range(chips):
        if final:
            for k in range(2):
                r = 2 * c + k
                out[r] = jnp.concatenate([s[4 * r : 4 * r + 4] for s in sums], axis=0)
        else:
            for side in range(3):
                n = c + side - 1
                piece = sums[0][8 * n : 8 * n + 8] if 0 <= n < chips else jnp.zeros((8, 128), F32)
                for k in range(2):
                    out[2 * c + k, pl.ds(8 * side, 8), :] = piece


def call(kernel, ins, outs, scratch=()):
    where = {"s": SMEM, "v": VMEM}
    return pl.pallas_call(
        kernel,
        out_shape=[jax.ShapeDtypeStruct(s, d) for s, d, _ in outs],
        in_specs=[pl.BlockSpec(memory_space=where[i]) for i in ins],
        out_specs=[pl.BlockSpec(memory_space=where[o]) for _, _, o in outs],
        scratch_shapes=[pltpu.VMEM(s, F32) for s in scratch],
        compiler_params=pltpu.CompilerParams(vmem_limit_bytes=16 * 1024 * 1024),
    )


def local(
    initial_field,
    conduct,
    velocity,
    heat_release,
    group_kind,
    partner,
    surface_cell,
    patch_count,
    patch_centres,
    patch_targets,
    patch_maps,
):
    subs = lax.axis_size("sub")
    groups = lax.axis_size("grp")
    block = surface_cell.shape[1]
    slots = patch_maps.shape[1]
    planes, cells = initial_field.shape[1:]

    fields = jnp.concatenate([initial_field, conduct, velocity, heat_release], axis=0)
    (payload,) = call(pack_kernel, "vv", [((1032, 128), F32, "v")])(fields, surface_cell)
    up = [(i, i + 2) for i in range(subs - 2)]
    down = [(i + 2, i) for i in range(subs - 2)]
    swap = [(i, i ^ 1) for i in range(subs)]
    cross = [(i, i + 1 if i % 2 else i - 1) for i in range(1, subs - 1)]
    left = lax.ppermute(payload, "sub", up)
    right = lax.ppermute(payload, "sub", down)
    mate = lax.ppermute(payload, "sub", swap)
    ints, flts, place, turned = call(
        prepare_kernel,
        "sssvv",
        [
            ((8, 128), jnp.int32, "v"),
            ((8, 128), F32, "v"),
            ((slots, 128), jnp.int32, "v"),
            ((slots, 128, 128), F32, "v"),
        ],
    )(group_kind, partner, patch_count, patch_centres[0], patch_maps[0])
    targets = patch_targets[0]
    left_mate = lax.ppermute(left, "sub", swap)
    right_mate = lax.ppermute(right, "sub", swap)

    keep_out = ((4 * ROWS + 8, 128), F32, "v")
    half_out = ((groups * subs, 4, 128), F32, "v")
    full_out = ((groups * subs, 8, 128), F32, "v")
    coef_shape = (3, WIDE - 2, ROWS, 128)
    work = [(WIDE, ROWS, 128), (WIDE, ROWS, 128), (2 * ROWS, 128)]
    keep, send, coef, surf = call(
        first_kernel,
        "vvvvvvv",
        [keep_out, half_out, (coef_shape, F32, "v"), ((6, 4, 128), jnp.int32, "v")],
        work,
    )(flts, payload, mate, left, left_mate, right, right_mate)
    for iteration in range(COUPLE):
        final = iteration == COUPLE - 1
        if not final:
            beside = lax.ppermute(keep, "sub", cross)
        source = lax.all_to_all(send, ("grp", "sub"), 0, 0, tiled=True)
        if not final:
            source, beside = lax.optimization_barrier((source, beside))
            other = lax.ppermute(beside, "sub", swap)
        (parts,) = call(
            functools.partial(patch_kernel, final=final),
            "vvvvv",
            [((subs, 8 if final else 24, 128), F32, "v")],
        )(ints, source, place, targets, turned)
        if not final:
            parts, other = lax.optimization_barrier((parts, other))
        parts = lax.all_to_all(parts, "sub", 0, 0, tiled=True)
        if final:
            field, interface = call(
                last_kernel, "vvvv", [((planes, cells), F32, "v"), ((2, block), F32, "v")]
            )(flts, parts, keep, surf)
        else:
            full = iteration == COUPLE - 2
            keep, send = call(
                functools.partial(middle_kernel, full=full),
                "vvvvvvv",
                [keep_out, full_out if full else half_out],
                work,
            )(flts, parts, keep, beside, other, surf, coef)
    return field[None], interface[None]


def solution(mesh):
    placed = (
        P("grp", "sub", None),
        P("grp", "sub", None),
        P("grp", "sub", None),
        P("grp", "sub", None),
        P(),
        P(),
        P("grp", "sub"),
        P("grp", None),
        P("grp", "sub", None),
        P("grp", "sub", None),
        P("grp", "sub", None, None),
    )
    return jax.shard_map(
        local,
        mesh=mesh,
        in_specs=placed,
        out_specs=(P("grp", "sub", None), P("grp", None, "sub")),
        check_vma=False,
    )
```

```python
import functools

import jax
import jax.numpy as jnp
from jax import lax
from jax.experimental import pallas as pl
from jax.experimental.pallas import tpu as pltpu
from jax.sharding import PartitionSpec as P


STEPS = 4
COUPLE = 4
ROWS = 128
HALO = 4
WIDE = 12
F32 = jnp.float32
BF16 = jnp.bfloat16
VMEM = pltpu.VMEM
SMEM = pltpu.SMEM


def iota(shape, dim):
    return lax.broadcasted_iota(jnp.int32, shape, dim)


def in_plane(x):
    above = jnp.concatenate([pltpu.roll(x[ROWS - 8 :], 1, 0), x[: ROWS - 8]], axis=0)
    below = jnp.concatenate([x[8:], pltpu.roll(x[:8], 7, 0)], axis=0)
    return (above + below) + (pltpu.roll(x, 1, 1) + pltpu.roll(x, 127, 1))


def run_steps(cur, nxt, coef):
    bufs = (cur, nxt)
    for step in range(STEPS):
        src, dst = bufs[step % 2], bufs[(step + 1) % 2]

        def body(p, carry, src=src, dst=dst):
            x = src[p]
            dst[p] = (
                x
                + coef[0, p - 1] * (src[p + 1] + in_plane(x) - 5.0 * x)
                + coef[1, p - 1] * (src[p - 1] - x)
                + coef[2, p - 1] * (1.0 + jnp.tanh(x))
            )
            return carry

        lax.fori_loop(step + 1, WIDE - 1 - step, body, 0, unroll=True)


def pick_nodes(jobs):
    keys = []
    for _, surf in jobs:
        lanes = [jnp.broadcast_to(surf[g : g + 1] & 127, (8, 128)) for g in range(4)]
        rows = [jnp.broadcast_to(surf[g : g + 1] >> 7, (8, 128)) - iota((8, 128), 0) for g in range(4)]
        keys.append((lanes, rows))

    def body(v, acc):
        out = []
        for (tables, _), (lanes, rows) in zip(jobs, keys):
            hits = [rows[g] == 8 * v for g in range(4)]
            for table in tables:
                tile = table(v)
                for g in range(4):
                    got = jnp.take_along_axis(tile, lanes[g], axis=1, mode="promise_in_bounds")
                    out.append(jnp.where(hits[g], got, acc[len(out)]))
        return tuple(out)

    total = sum(len(tables) for tables, _ in jobs)
    acc = lax.fori_loop(0, 32, body, tuple(jnp.zeros((8, 128), F32) for _ in range(4 * total)), unroll=8)
    return [
        jnp.concatenate([jnp.sum(acc[4 * t + g], axis=0, keepdims=True) for g in range(4)], axis=0)
        for t in range(total)
    ]


def halves(x):
    high = x.astype(BF16)
    return high, (x - high.astype(F32)).astype(BF16)


def rows_at(index, count):
    return iota((count, 128), 0).astype(F32).astype(BF16) == index.astype(F32).astype(BF16)


def one_hot(index, count):
    return jnp.where(rows_at(index, count), jnp.bfloat16(1), jnp.bfloat16(0))


def spread(index, value):
    hit = rows_at(index, 128)
    return jnp.concatenate([jnp.where(hit, part, jnp.bfloat16(0)) for part in halves(value)], axis=0)


def product(left, right):
    out = lax.dot_general(
        jnp.concatenate(left, axis=1),
        jnp.concatenate(right, axis=1),
        (((1,), (1,)), ((), ())),
        preferred_element_type=F32,
    )
    return out[:, :128] + out[:, 128:]


def scatter_block(surf, inc):
    groups = [slice(g, g + 1) for g in range(4)]
    return product(
        [one_hot(surf[g] >> 7, 256) for g in groups], [spread(surf[g] & 127, inc[g]) for g in groups]
    )


def finish(flts, cur, coef, surf_ref, flux, keep, export, full):
    core = lax.axis_index("sub") & 1
    for p in range(4):
        keep[pl.ds(p * ROWS, ROWS), :] = cur[HALO + p]
    for p in range(2):
        x = cur[HALO + 2 * core + p]
        flux[pl.ds(p * ROWS, ROWS), :] = coef[0, HALO - 1 + 2 * core + p] * (4.0 * x - in_plane(x))

    def plane_tile(first):
        def tile(v):
            return cur[first + v // 16, pl.ds(pl.multiple_of((v % 16) * 8, 8), 8), :]

        return tile

    def flux_tile(v):
        return flux[pl.ds(pl.multiple_of(v * 8, 8), 8), :]

    own, own_flux, mate = pick_nodes(
        [
            ([plane_tile(HALO + 2 * core), flux_tile], surf_ref[pl.ds(2 + core, 1)][0]),
            ([plane_tile(HALO + 2 - 2 * core)], surf_ref[pl.ds(3 - core, 1)][0]),
        ]
    )
    is_first = core == 0
    keep[pl.ds(4 * ROWS, 8), :] = jnp.concatenate(
        [jnp.where(is_first, own, mate), jnp.where(is_first, mate, own)], axis=0
    )
    if full:
        block = jnp.concatenate([own, own_flux], axis=0)
    else:
        block = flts[3:4, :] * own + flts[4:5, :] * own_flux
    export[...] = jnp.broadcast_to(block[None], export.shape)


def pack_kernel(fields, surface, payload):
    for i in range(4):
        rows = fields[i].reshape(2 * ROWS, 128)
        for p in range(2):
            for lane in range(8):
                start = p * ROWS + 16 * lane
                payload[pl.ds(256 * i + p * ROWS + lane, 16, stride=8), :] = rows[start : start + 16]
    cells = surface[...].reshape(4, 128)
    row = (cells >> 7) & (ROWS - 1)
    kept = ((row & 15) << 3) | (row >> 4)
    cells = ((cells & ~(127 << 7)) | (kept << 7)).astype(F32)
    payload[pl.ds(1024, 8), :] = jnp.concatenate([cells, cells], axis=0)


def prepare_kernel(kinds, partners, counts, centres, maps, ints, flts, place, turned):
    group = lax.axis_index("grp")
    me = lax.axis_index("sub")
    subs = counts.shape[1]
    nodes = subs * 512
    live = counts[0, me]
    kind = kinds[group]
    at = centres[...]
    anchor = at[0:1, 0:1]
    apart = ((at - anchor + nodes // 2) & (nodes - 1)) - nodes // 2
    apart = jnp.where(iota(at.shape, 0) < live, apart, 0)
    lowest = jnp.min(apart.astype(F32)).astype(jnp.int32)
    start = (jnp.max(anchor.astype(F32)).astype(jnp.int32) + lowest) & (nodes - 1)
    first = start >> 9
    place[...] = jnp.where(iota(at.shape, 0) < live, (at - first * 512) & (nodes - 1), -1)
    ints[...] = jnp.full(ints.shape, partners[group] * subs + first, jnp.int32)
    is_gas = kind == 0
    for row, (gas, solid) in enumerate(((0.5, 0.25), (-0.25, 0.25), (1.0, 0.0), (0.25, 0.5), (0.25, -0.25))):
        flts[pl.ds(row, 1), :] = jnp.full((1, 128), jnp.where(is_gas, gas, solid), F32)
    for s in range(maps.shape[0]):
        turned[s] = maps[s].T


def first_kernel(flts, own, mate, left, left_mate, right, right_mate,
                 keep, export, coef, surf, cur, nxt, flux):
    core = lax.axis_index("sub") & 1
    other = 1 - core
    for base, mine, its in ((0, left, left_mate), (4, own, mate), (8, right, right_mate)):
        for p in range(2):
            cur[base + 2 * core + p] = mine[pl.ds(p * ROWS, ROWS), :]
            cur[base + 2 * other + p] = its[pl.ds(p * ROWS, ROWS), :]
        tail = mine[pl.ds(1024, 8), :].astype(jnp.int32)
        tail_mate = its[pl.ds(1024, 8), :].astype(jnp.int32)
        surf[pl.ds(base // 2 + core, 1)] = tail[:4][None]
        surf[pl.ds(base // 2 + other, 1)] = tail_mate[:4][None]
    gas = flts[2:3, :]

    def store(p, ref, half):
        got = [ref[pl.ds(256 * (w + 1) + half * ROWS, ROWS), :] for w in range(3)]
        coef[0, p] = got[0]
        coef[1, p] = got[0] + gas * got[1]
        coef[2, p] = (0.5 * gas) * got[2]

    for half in range(2):
        store(3 + 2 * core + half, own, half)
        store(3 + 2 * other + half, mate, half)

    @pl.when(core == 0)
    def _():
        store(0, left, 1)
        store(1, left_mate, 0)
        store(2, left_mate, 1)
        store(7, right, 0)
        store(8, right, 1)
        store(9, right_mate, 0)

    @pl.when(core == 1)
    def _():
        store(0, left_mate, 1)
        store(1, left, 0)
        store(2, left, 1)
        store(7, right_mate, 0)
        store(8, right_mate, 1)
        store(9, right, 0)

    run_steps(cur, nxt, coef)
    finish(flts, cur, coef, surf, flux, keep, export, False)


def middle_kernel(flts, parts, own, beside, other, surf, coef, keep, export,
                  cur, nxt, flux, *, full):
    first = (lax.axis_index("sub") & 1) == 0
    total = sum_parts(parts)

    def sides(start, size):
        near = beside[pl.ds(start, size), :]
        far = other[pl.ds(start, size), :]
        return jnp.where(first, near, far), own[pl.ds(start, size), :], jnp.where(first, far, near)

    temps = sides(4 * ROWS, 8)
    incs = [total[8 * side : 8 * side + 8] - flts[0:1, :] * temps[side] for side in range(3)]
    for half in range(2):
        planes = sides(2 * half * ROWS, 2 * ROWS)
        for side in range(3):
            block = 2 * side + half
            out = planes[side] + scatter_block(surf[block], incs[side][4 * half : 4 * half + 4])
            cur[2 * block] = out[:ROWS]
            cur[2 * block + 1] = out[ROWS:]
    run_steps(cur, nxt, coef)
    finish(flts, cur, coef, surf, flux, keep, export, full)


def sum_parts(parts):
    lanes = [parts[i] for i in range(4)]
    for i in range(4, parts.shape[0]):
        lanes[i % 4] = lanes[i % 4] + parts[i]
    return (lanes[0] + lanes[1]) + (lanes[2] + lanes[3])


def last_kernel(flts, parts, own, surf, field, interface, work):
    core = lax.axis_index("sub") & 1
    total = sum_parts(parts)
    interface[...] = total.reshape(2, 512)
    temps = own[pl.ds(4 * ROWS, 8), :]
    temps = jnp.where(core == 0, temps[:4], temps[4:])
    inc = flts[0:1, :] * (total[:4] - temps) + flts[1:2, :] * total[4:]
    add = scatter_block(surf[pl.ds(2 + core, 1)][0], inc)
    start = pl.multiple_of(core * 2 * ROWS, 2 * ROWS)
    work[...] = own[pl.ds(start, 2 * ROWS), :] + add
    rows = [work[pl.ds(p * ROWS + lane, 16, stride=8), :] for p in range(2) for lane in range(8)]
    field[...] = jnp.concatenate(rows, axis=0).reshape(2, 128 * ROWS)


def patch_kernel(ints, source, place, targets, maps, out, *, final):
    slots = place.shape[0]
    subs = out.shape[0]
    parts = 2 if final else 1
    lanes = [place[pl.ds(8 * w, 8), :] & 127 for w in range(slots // 8)]
    rows = [place[pl.ds(8 * w, 8), :] >> 7 for w in range(slots // 8)]
    vals = [[jnp.zeros((8, 128), F32) for _ in rows] for _ in range(parts)]
    at = jnp.max(ints[0:1, :].astype(F32)).astype(jnp.int32)
    for i in range(3):
        tile = source[(at & -subs) + ((at + i) & (subs - 1))]
        for q in range(parts):
            for j in range(4):
                line = jnp.broadcast_to(tile[4 * q + j : 4 * q + j + 1], (8, 128))
                for w in range(slots // 8):
                    got = jnp.take_along_axis(line, lanes[w], axis=1, mode="promise_in_bounds")
                    vals[q][w] = jnp.where(rows[w] == 4 * i + j, got, vals[q][w])
    columns = []
    for q in range(parts):
        full = jnp.concatenate(vals[q] + [jnp.zeros((128 - slots, 128), F32)], axis=0)
        columns.append(full.T)
    left, right = [], [[] for _ in range(parts)]
    for s in range(slots):
        aim = targets[s : s + 1, :]
        left.append(one_hot(aim >> 7, 128))
        table = maps[s]
        for q in range(parts):
            value = jnp.sum(table * columns[q][:, s : s + 1], axis=0, keepdims=True)
            right[q].append(spread(aim & 127, value))
    sums = [product(left, right[q]) for q in range(parts)]
    chips = out.shape[0] // 2
    for c in range(chips):
        if final:
            for k in range(2):
                r = 2 * c + k
                out[r] = jnp.concatenate([s[4 * r : 4 * r + 4] for s in sums], axis=0)
        else:
            for side in range(3):
                n = c + side - 1
                piece = sums[0][8 * n : 8 * n + 8] if 0 <= n < chips else jnp.zeros((8, 128), F32)
                for k in range(2):
                    out[2 * c + k, pl.ds(8 * side, 8), :] = piece


def call(kernel, ins, outs, scratch=()):
    where = {"s": SMEM, "v": VMEM}
    return pl.pallas_call(
        kernel,
        out_shape=[jax.ShapeDtypeStruct(s, d) for s, d, _ in outs],
        in_specs=[pl.BlockSpec(memory_space=where[i]) for i in ins],
        out_specs=[pl.BlockSpec(memory_space=where[o]) for _, _, o in outs],
        scratch_shapes=[pltpu.VMEM(s, F32) for s in scratch],
        compiler_params=pltpu.CompilerParams(vmem_limit_bytes=16 * 1024 * 1024),
    )


def local(
    initial_field,
    conduct,
    velocity,
    heat_release,
    group_kind,
    partner,
    surface_cell,
    patch_count,
    patch_centres,
    patch_targets,
    patch_maps,
):
    subs = lax.axis_size("sub")
    groups = lax.axis_size("grp")
    block = surface_cell.shape[1]
    slots = patch_maps.shape[1]
    planes, cells = initial_field.shape[1:]

    fields = jnp.concatenate([initial_field, conduct, velocity, heat_release], axis=0)
    (payload,) = call(pack_kernel, "vv", [((1032, 128), F32, "v")])(fields, surface_cell)
    up = [(i, i + 2) for i in range(subs - 2)]
    down = [(i + 2, i) for i in range(subs - 2)]
    swap = [(i, i ^ 1) for i in range(subs)]
    cross = [(i, i + 1 if i % 2 else i - 1) for i in range(1, subs - 1)]
    left = lax.ppermute(payload, "sub", up)
    right = lax.ppermute(payload, "sub", down)
    mate = lax.ppermute(payload, "sub", swap)
    ints, flts, place, turned = call(
        prepare_kernel,
        "sssvv",
        [
            ((8, 128), jnp.int32, "v"),
            ((8, 128), F32, "v"),
            ((slots, 128), jnp.int32, "v"),
            ((slots, 128, 128), F32, "v"),
        ],
    )(group_kind, partner, patch_count, patch_centres[0], patch_maps[0])
    targets = patch_targets[0]
    left_mate = lax.ppermute(left, "sub", swap)
    right_mate = lax.ppermute(right, "sub", swap)

    keep_out = ((4 * ROWS + 8, 128), F32, "v")
    half_out = ((groups * subs, 4, 128), F32, "v")
    full_out = ((groups * subs, 8, 128), F32, "v")
    coef_shape = (3, WIDE - 2, ROWS, 128)
    work = [(WIDE, ROWS, 128), (WIDE, ROWS, 128), (2 * ROWS, 128)]
    keep, send, coef, surf = call(
        first_kernel,
        "vvvvvvv",
        [keep_out, half_out, (coef_shape, F32, "v"), ((6, 4, 128), jnp.int32, "v")],
        work,
    )(flts, payload, mate, left, left_mate, right, right_mate)
    for iteration in range(COUPLE):
        final = iteration == COUPLE - 1
        if not final:
            beside = lax.ppermute(keep, "sub", cross)
        source = lax.all_to_all(send, ("grp", "sub"), 0, 0, tiled=True)
        if not final:
            source, beside = lax.optimization_barrier((source, beside))
            other = lax.ppermute(beside, "sub", swap)
        (parts,) = call(
            functools.partial(patch_kernel, final=final),
            "vvvvv",
            [((subs, 8 if final else 24, 128), F32, "v")],
        )(ints, source, place, targets, turned)
        if not final:
            parts, other = lax.optimization_barrier((parts, other))
        parts = lax.all_to_all(parts, "sub", 0, 0, tiled=True)
        if final:
            field, interface = call(
                last_kernel,
                "vvvv",
                [((planes, cells), F32, "v"), ((2, block), F32, "v")],
                [(2 * ROWS, 128)],
            )(flts, parts, keep, surf)
        else:
            full = iteration == COUPLE - 2
            keep, send = call(
                functools.partial(middle_kernel, full=full),
                "vvvvvvv",
                [keep_out, full_out if full else half_out],
                work,
            )(flts, parts, keep, beside, other, surf, coef)
    return field[None], interface[None]


def solution(mesh):
    placed = (
        P("grp", "sub", None),
        P("grp", "sub", None),
        P("grp", "sub", None),
        P("grp", "sub", None),
        P(),
        P(),
        P("grp", "sub"),
        P("grp", None),
        P("grp", "sub", None),
        P("grp", "sub", None),
        P("grp", "sub", None, None),
    )
    return jax.shard_map(
        local,
        mesh=mesh,
        in_specs=placed,
        out_specs=(P("grp", "sub", None), P("grp", None, "sub")),
        check_vma=False,
    )
```

```python
import functools

import jax
import jax.numpy as jnp
from jax import lax
from jax.experimental import pallas as pl
from jax.experimental.pallas import tpu as pltpu
from jax.sharding import PartitionSpec as P


STEPS = 4
COUPLE = 4
ROWS = 128
HALO = 4
WIDE = 12
F32 = jnp.float32
BF16 = jnp.bfloat16
VMEM = pltpu.VMEM
SMEM = pltpu.SMEM


def iota(shape, dim):
    return lax.broadcasted_iota(jnp.int32, shape, dim)


def in_plane(x):
    above = jnp.concatenate([pltpu.roll(x[ROWS - 8 :], 1, 0), x[: ROWS - 8]], axis=0)
    below = jnp.concatenate([x[8:], pltpu.roll(x[:8], 7, 0)], axis=0)
    return (above + below) + (pltpu.roll(x, 1, 1) + pltpu.roll(x, 127, 1))


def run_steps(cur, nxt, coef):
    bufs = (cur, nxt)
    for step in range(STEPS):
        src, dst = bufs[step % 2], bufs[(step + 1) % 2]

        def body(p, carry, src=src, dst=dst):
            x = src[p]
            dst[p] = (
                x
                + coef[0, p - 1] * (src[p + 1] + in_plane(x) - 5.0 * x)
                + coef[1, p - 1] * (src[p - 1] - x)
                + coef[2, p - 1] * (1.0 + jnp.tanh(x))
            )
            return carry

        lax.fori_loop(step + 1, WIDE - 1 - step, body, 0, unroll=True)


def pick_nodes(jobs):
    keys = []
    for _, surf in jobs:
        lanes = [jnp.broadcast_to(surf[g : g + 1] & 127, (8, 128)) for g in range(4)]
        rows = [jnp.broadcast_to(surf[g : g + 1] >> 7, (8, 128)) - iota((8, 128), 0) for g in range(4)]
        keys.append((lanes, rows))

    def body(v, acc):
        out = []
        for (tables, _), (lanes, rows) in zip(jobs, keys):
            hits = [rows[g] == 8 * v for g in range(4)]
            for table in tables:
                tile = table(v)
                for g in range(4):
                    got = jnp.take_along_axis(tile, lanes[g], axis=1, mode="promise_in_bounds")
                    out.append(jnp.where(hits[g], got, acc[len(out)]))
        return tuple(out)

    total = sum(len(tables) for tables, _ in jobs)
    acc = lax.fori_loop(0, 32, body, tuple(jnp.zeros((8, 128), F32) for _ in range(4 * total)), unroll=8)
    return [
        jnp.concatenate([jnp.sum(acc[4 * t + g], axis=0, keepdims=True) for g in range(4)], axis=0)
        for t in range(total)
    ]


def halves(x):
    high = x.astype(BF16)
    return high, (x - high.astype(F32)).astype(BF16)


def rows_at(index, count):
    return iota((count, 128), 0).astype(F32).astype(BF16) == index.astype(F32).astype(BF16)


def one_hot(index, count):
    return jnp.where(rows_at(index, count), jnp.bfloat16(1), jnp.bfloat16(0))


def spread(index, value):
    hit = rows_at(index, 128)
    return jnp.concatenate([jnp.where(hit, part, jnp.bfloat16(0)) for part in halves(value)], axis=0)


def product(left, right):
    out = lax.dot_general(
        jnp.concatenate(left, axis=1),
        jnp.concatenate(right, axis=1),
        (((1,), (1,)), ((), ())),
        preferred_element_type=F32,
    )
    return out[:, :128] + out[:, 128:]


def scatter_block(surf, inc):
    groups = [slice(g, g + 1) for g in range(4)]
    return product(
        [one_hot(surf[g] >> 7, 256) for g in groups], [spread(surf[g] & 127, inc[g]) for g in groups]
    )


def finish(flts, cur, coef, surf_ref, flux, keep, export, full):
    core = lax.axis_index("sub") & 1
    for p in range(4):
        keep[pl.ds(p * ROWS, ROWS), :] = cur[HALO + p]
    for p in range(2):
        x = cur[HALO + 2 * core + p]
        flux[pl.ds(p * ROWS, ROWS), :] = coef[0, HALO - 1 + 2 * core + p] * (4.0 * x - in_plane(x))

    def plane_tile(first):
        def tile(v):
            return cur[first + v // 16, pl.ds(pl.multiple_of((v % 16) * 8, 8), 8), :]

        return tile

    def flux_tile(v):
        return flux[pl.ds(pl.multiple_of(v * 8, 8), 8), :]

    own, own_flux, mate = pick_nodes(
        [
            ([plane_tile(HALO + 2 * core), flux_tile], surf_ref[pl.ds(2 + core, 1)][0]),
            ([plane_tile(HALO + 2 - 2 * core)], surf_ref[pl.ds(3 - core, 1)][0]),
        ]
    )
    is_first = core == 0
    keep[pl.ds(4 * ROWS, 8), :] = jnp.concatenate(
        [jnp.where(is_first, own, mate), jnp.where(is_first, mate, own)], axis=0
    )
    if full:
        block = jnp.concatenate([own, own_flux], axis=0)
    else:
        block = flts[3:4, :] * own + flts[4:5, :] * own_flux
    export[...] = jnp.broadcast_to(block[None], export.shape)


def pack_kernel(fields, surface, payload):
    for i in range(4):
        rows = fields[i].reshape(2 * ROWS, 128)
        for p in range(2):
            for lane in range(8):
                start = p * ROWS + 16 * lane
                payload[pl.ds(256 * i + p * ROWS + lane, 16, stride=8), :] = rows[start : start + 16]
    cells = surface[...].reshape(4, 128)
    row = (cells >> 7) & (ROWS - 1)
    kept = ((row & 15) << 3) | (row >> 4)
    cells = ((cells & ~(127 << 7)) | (kept << 7)).astype(F32)
    payload[pl.ds(1024, 8), :] = jnp.concatenate([cells, cells], axis=0)


def prepare_kernel(kinds, partners, counts, centres, maps, ints, flts, place, turned):
    group = lax.axis_index("grp")
    me = lax.axis_index("sub")
    subs = counts.shape[1]
    nodes = subs * 512
    live = counts[0, me]
    kind = kinds[group]
    at = centres[...]
    anchor = at[0:1, 0:1]
    apart = ((at - anchor + nodes // 2) & (nodes - 1)) - nodes // 2
    apart = jnp.where(iota(at.shape, 0) < live, apart, 0)
    lowest = jnp.min(apart.astype(F32)).astype(jnp.int32)
    start = (jnp.max(anchor.astype(F32)).astype(jnp.int32) + lowest) & (nodes - 1)
    first = start >> 9
    place[...] = jnp.where(iota(at.shape, 0) < live, (at - first * 512) & (nodes - 1), -1)
    ints[...] = jnp.full(ints.shape, partners[group] * subs + first, jnp.int32)
    is_gas = kind == 0
    for row, (gas, solid) in enumerate(((0.5, 0.25), (-0.25, 0.25), (1.0, 0.0), (0.25, 0.5), (0.25, -0.25))):
        flts[pl.ds(row, 1), :] = jnp.full((1, 128), jnp.where(is_gas, gas, solid), F32)
    for s in range(maps.shape[0]):
        turned[s] = maps[s].T


def far_kernel(mate, far):
    skip = jnp.where((lax.axis_index("sub") & 1) == 0, 0, ROWS)
    far[pl.ds(0, 2 * ROWS), :] = mate[pl.ds(0, 2 * ROWS), :]
    for which in range(3):
        start = pl.multiple_of(256 * (which + 1) + skip, ROWS)
        far[pl.ds((2 + which) * ROWS, ROWS), :] = mate[pl.ds(start, ROWS), :]
    far[pl.ds(5 * ROWS, 8), :] = mate[pl.ds(1024, 8), :]


def first_kernel(flts, own, mate, near, near_other, far, far_other,
                 keep, export, coef, surf, cur, nxt, flux):
    first = (lax.axis_index("sub") & 1) == 0
    gas = flts[2:3, :]

    def pick(one, other, start, size):
        x = one[pl.ds(start, size), :]
        y = other[pl.ds(start, size), :]
        return jnp.where(first, x, y), jnp.where(first, y, x)

    pairs = ((far, far_other, 5 * ROWS, (0, 5)), (near, near_other, 1024, (1, 4)), (own, mate, 1024, (2, 3)))
    for one, other, tail, blocks in pairs:
        both = pick(one, other, 0, 2 * ROWS)
        cells = pick(one, other, tail, 8)
        for side, block in enumerate(blocks):
            cur[2 * block] = both[side][:ROWS]
            cur[2 * block + 1] = both[side][ROWS:]
            surf[block] = cells[side][:4].astype(jnp.int32)

    def store(one, other, starts, planes):
        got = [pick(one, other, start, ROWS) for start in starts]
        for side, plane in enumerate(planes):
            conduct, velocity, heat = (g[side] for g in got)
            coef[0, plane - 1] = conduct
            coef[1, plane - 1] = conduct + gas * velocity
            coef[2, plane - 1] = (0.5 * gas) * heat

    for half in range(2):
        starts = [256 * (w + 1) + half * ROWS for w in range(3)]
        store(own, mate, starts, (4 + half, 6 + half))
        store(near, near_other, starts, (2 + half, 8 + half))
    store(far, far_other, [(2 + w) * ROWS for w in range(3)], (1, 10))
    run_steps(cur, nxt, coef)
    finish(flts, cur, coef, surf, flux, keep, export, False)


def middle_kernel(flts, parts, own, beside, other, surf, coef, keep, export,
                  cur, nxt, flux, *, full):
    first = (lax.axis_index("sub") & 1) == 0
    total = sum_parts(parts)

    def sides(start, size):
        near = beside[pl.ds(start, size), :]
        far = other[pl.ds(start, size), :]
        return jnp.where(first, near, far), own[pl.ds(start, size), :], jnp.where(first, far, near)

    temps = sides(4 * ROWS, 8)
    incs = [total[8 * side : 8 * side + 8] - flts[0:1, :] * temps[side] for side in range(3)]
    for half in range(2):
        planes = sides(2 * half * ROWS, 2 * ROWS)
        for side in range(3):
            block = 2 * side + half
            out = planes[side] + scatter_block(surf[block], incs[side][4 * half : 4 * half + 4])
            cur[2 * block] = out[:ROWS]
            cur[2 * block + 1] = out[ROWS:]
    run_steps(cur, nxt, coef)
    finish(flts, cur, coef, surf, flux, keep, export, full)


def sum_parts(parts):
    lanes = [parts[i] for i in range(4)]
    for i in range(4, parts.shape[0]):
        lanes[i % 4] = lanes[i % 4] + parts[i]
    return (lanes[0] + lanes[1]) + (lanes[2] + lanes[3])


def last_kernel(flts, parts, own, surf, field, interface, work):
    core = lax.axis_index("sub") & 1
    total = sum_parts(parts)
    interface[...] = total.reshape(2, 512)
    temps = own[pl.ds(4 * ROWS, 8), :]
    temps = jnp.where(core == 0, temps[:4], temps[4:])
    inc = flts[0:1, :] * (total[:4] - temps) + flts[1:2, :] * total[4:]
    add = scatter_block(surf[pl.ds(2 + core, 1)][0], inc)
    start = pl.multiple_of(core * 2 * ROWS, 2 * ROWS)
    work[...] = own[pl.ds(start, 2 * ROWS), :] + add
    rows = [work[pl.ds(p * ROWS + lane, 16, stride=8), :] for p in range(2) for lane in range(8)]
    field[...] = jnp.concatenate(rows, axis=0).reshape(2, 128 * ROWS)


def patch_kernel(ints, source, place, targets, maps, out, *, final):
    slots = place.shape[0]
    subs = out.shape[0]
    parts = 2 if final else 1
    lanes = [place[pl.ds(8 * w, 8), :] & 127 for w in range(slots // 8)]
    rows = [place[pl.ds(8 * w, 8), :] >> 7 for w in range(slots // 8)]
    vals = [[jnp.zeros((8, 128), F32) for _ in rows] for _ in range(parts)]
    at = jnp.max(ints[0:1, :].astype(F32)).astype(jnp.int32)
    for i in range(3):
        tile = source[(at & -subs) + ((at + i) & (subs - 1))]
        for q in range(parts):
            for j in range(4):
                line = jnp.broadcast_to(tile[4 * q + j : 4 * q + j + 1], (8, 128))
                for w in range(slots // 8):
                    got = jnp.take_along_axis(line, lanes[w], axis=1, mode="promise_in_bounds")
                    vals[q][w] = jnp.where(rows[w] == 4 * i + j, got, vals[q][w])
    columns = []
    for q in range(parts):
        full = jnp.concatenate(vals[q] + [jnp.zeros((128 - slots, 128), F32)], axis=0)
        columns.append(full.T)
    left, right = [], [[] for _ in range(parts)]
    for s in range(slots):
        aim = targets[s : s + 1, :]
        left.append(one_hot(aim >> 7, 128))
        table = maps[s]
        for q in range(parts):
            value = jnp.sum(table * columns[q][:, s : s + 1], axis=0, keepdims=True)
            right[q].append(spread(aim & 127, value))
    sums = [product(left, right[q]) for q in range(parts)]
    chips = out.shape[0] // 2
    for c in range(chips):
        if final:
            for k in range(2):
                r = 2 * c + k
                out[r] = jnp.concatenate([s[4 * r : 4 * r + 4] for s in sums], axis=0)
        else:
            for side in range(3):
                n = c + side - 1
                piece = sums[0][8 * n : 8 * n + 8] if 0 <= n < chips else jnp.zeros((8, 128), F32)
                for k in range(2):
                    out[2 * c + k, pl.ds(8 * side, 8), :] = piece


def call(kernel, ins, outs, scratch=()):
    where = {"s": SMEM, "v": VMEM}
    return pl.pallas_call(
        kernel,
        out_shape=[jax.ShapeDtypeStruct(s, d) for s, d, _ in outs],
        in_specs=[pl.BlockSpec(memory_space=where[i]) for i in ins],
        out_specs=[pl.BlockSpec(memory_space=where[o]) for _, _, o in outs],
        scratch_shapes=[pltpu.VMEM(s, F32) for s in scratch],
        compiler_params=pltpu.CompilerParams(vmem_limit_bytes=16 * 1024 * 1024),
    )


def local(
    initial_field,
    conduct,
    velocity,
    heat_release,
    group_kind,
    partner,
    surface_cell,
    patch_count,
    patch_centres,
    patch_targets,
    patch_maps,
):
    subs = lax.axis_size("sub")
    groups = lax.axis_size("grp")
    block = surface_cell.shape[1]
    slots = patch_maps.shape[1]
    planes, cells = initial_field.shape[1:]

    fields = jnp.concatenate([initial_field, conduct, velocity, heat_release], axis=0)
    (payload,) = call(pack_kernel, "vv", [((1032, 128), F32, "v")])(fields, surface_cell)
    swap = [(i, i ^ 1) for i in range(subs)]
    cross = [(i, i + 1 if i % 2 else i - 1) for i in range(1, subs - 1)]
    near = lax.ppermute(payload, "sub", cross)
    mate = lax.ppermute(payload, "sub", swap)
    (far,) = call(far_kernel, "v", [((5 * ROWS + 8, 128), F32, "v")])(mate)
    far = lax.ppermute(far, "sub", cross)
    ints, flts, place, turned = call(
        prepare_kernel,
        "sssvv",
        [
            ((8, 128), jnp.int32, "v"),
            ((8, 128), F32, "v"),
            ((slots, 128), jnp.int32, "v"),
            ((slots, 128, 128), F32, "v"),
        ],
    )(group_kind, partner, patch_count, patch_centres[0], patch_maps[0])
    targets = patch_targets[0]
    near_other = lax.ppermute(near, "sub", swap)
    far_other = lax.ppermute(far, "sub", swap)

    keep_out = ((4 * ROWS + 8, 128), F32, "v")
    half_out = ((groups * subs, 4, 128), F32, "v")
    full_out = ((groups * subs, 8, 128), F32, "v")
    coef_shape = (3, WIDE - 2, ROWS, 128)
    work = [(WIDE, ROWS, 128), (WIDE, ROWS, 128), (2 * ROWS, 128)]
    keep, send, coef, surf = call(
        first_kernel,
        "vvvvvvv",
        [keep_out, half_out, (coef_shape, F32, "v"), ((6, 4, 128), jnp.int32, "v")],
        work,
    )(flts, payload, mate, near, near_other, far, far_other)
    for iteration in range(COUPLE):
        final = iteration == COUPLE - 1
        if not final:
            beside = lax.ppermute(keep, "sub", cross)
        source = lax.all_to_all(send, ("grp", "sub"), 0, 0, tiled=True)
        if not final:
            source, beside = lax.optimization_barrier((source, beside))
            other = lax.ppermute(beside, "sub", swap)
        (parts,) = call(
            functools.partial(patch_kernel, final=final),
            "vvvvv",
            [((subs, 8 if final else 24, 128), F32, "v")],
        )(ints, source, place, targets, turned)
        if not final:
            parts, other = lax.optimization_barrier((parts, other))
        parts = lax.all_to_all(parts, "sub", 0, 0, tiled=True)
        if final:
            field, interface = call(
                last_kernel,
                "vvvv",
                [((planes, cells), F32, "v"), ((2, block), F32, "v")],
                [(2 * ROWS, 128)],
            )(flts, parts, keep, surf)
        else:
            full = iteration == COUPLE - 2
            keep, send = call(
                functools.partial(middle_kernel, full=full),
                "vvvvvvv",
                [keep_out, full_out if full else half_out],
                work,
            )(flts, parts, keep, beside, other, surf, coef)
    return field[None], interface[None]


def solution(mesh):
    placed = (
        P("grp", "sub", None),
        P("grp", "sub", None),
        P("grp", "sub", None),
        P("grp", "sub", None),
        P(),
        P(),
        P("grp", "sub"),
        P("grp", None),
        P("grp", "sub", None),
        P("grp", "sub", None),
        P("grp", "sub", None, None),
    )
    return jax.shard_map(
        local,
        mesh=mesh,
        in_specs=placed,
        out_specs=(P("grp", "sub", None), P("grp", None, "sub")),
        check_vma=False,
    )
```

```python
import functools

import jax
import jax.numpy as jnp
from jax import lax
from jax.experimental import pallas as pl
from jax.experimental.pallas import tpu as pltpu
from jax.sharding import PartitionSpec as P


STEPS = 4
COUPLE = 4
ROWS = 128
HALO = 4
WIDE = 12
F32 = jnp.float32
BF16 = jnp.bfloat16
VMEM = pltpu.VMEM
SMEM = pltpu.SMEM


def iota(shape, dim):
    return lax.broadcasted_iota(jnp.int32, shape, dim)


def in_plane(x):
    above = jnp.concatenate([pltpu.roll(x[ROWS - 8 :], 1, 0), x[: ROWS - 8]], axis=0)
    below = jnp.concatenate([x[8:], pltpu.roll(x[:8], 7, 0)], axis=0)
    return (above + below) + (pltpu.roll(x, 1, 1) + pltpu.roll(x, 127, 1))


def run_steps(cur, nxt, coef):
    bufs = (cur, nxt)
    for step in range(STEPS):
        src, dst = bufs[step % 2], bufs[(step + 1) % 2]

        def body(p, carry, src=src, dst=dst):
            x = src[p]
            near = src[p + 1] + in_plane(x)
            dst[p] = (coef[3, p - 1] * x + coef[0, p - 1] * near) + (
                coef[1, p - 1] * src[p - 1] + coef[2, p - 1] * (1.0 + jnp.tanh(x))
            )
            return carry

        lax.fori_loop(step + 1, WIDE - 1 - step, body, 0, unroll=True)


def pick_nodes(jobs):
    keys = []
    for _, surf in jobs:
        lanes = [jnp.broadcast_to(surf[g : g + 1] & 127, (8, 128)) for g in range(4)]
        rows = [jnp.broadcast_to(surf[g : g + 1] >> 7, (8, 128)) - iota((8, 128), 0) for g in range(4)]
        keys.append((lanes, rows))

    def body(v, acc):
        out = []
        for (tables, _), (lanes, rows) in zip(jobs, keys):
            hits = [rows[g] == 8 * v for g in range(4)]
            for table in tables:
                tile = table(v)
                for g in range(4):
                    got = jnp.take_along_axis(tile, lanes[g], axis=1, mode="promise_in_bounds")
                    out.append(jnp.where(hits[g], got, acc[len(out)]))
        return tuple(out)

    total = sum(len(tables) for tables, _ in jobs)
    acc = lax.fori_loop(0, 32, body, tuple(jnp.zeros((8, 128), F32) for _ in range(4 * total)), unroll=8)
    return [
        jnp.concatenate([jnp.sum(acc[4 * t + g], axis=0, keepdims=True) for g in range(4)], axis=0)
        for t in range(total)
    ]


def halves(x):
    high = x.astype(BF16)
    return high, (x - high.astype(F32)).astype(BF16)


def rows_at(index, count):
    return iota((count, 128), 0).astype(F32).astype(BF16) == index.astype(F32).astype(BF16)


def one_hot(index, count):
    return jnp.where(rows_at(index, count), jnp.bfloat16(1), jnp.bfloat16(0))


def spread(index, value):
    hit = rows_at(index, 128)
    return jnp.concatenate([jnp.where(hit, part, jnp.bfloat16(0)) for part in halves(value)], axis=0)


def product(left, right):
    out = lax.dot_general(
        jnp.concatenate(left, axis=1),
        jnp.concatenate(right, axis=1),
        (((1,), (1,)), ((), ())),
        preferred_element_type=F32,
    )
    return out[:, :128] + out[:, 128:]


def scatter_block(surf, inc):
    groups = [slice(g, g + 1) for g in range(4)]
    return product(
        [one_hot(surf[g] >> 7, 256) for g in groups], [spread(surf[g] & 127, inc[g]) for g in groups]
    )


def finish(flts, cur, coef, surf_ref, flux, keep, export, full):
    core = lax.axis_index("sub") & 1
    for p in range(4):
        keep[pl.ds(p * ROWS, ROWS), :] = cur[HALO + p]
    for p in range(2):
        x = cur[HALO + 2 * core + p]
        flux[pl.ds(p * ROWS, ROWS), :] = coef[0, HALO - 1 + 2 * core + p] * (4.0 * x - in_plane(x))

    def plane_tile(first):
        def tile(v):
            return cur[first + v // 16, pl.ds(pl.multiple_of((v % 16) * 8, 8), 8), :]

        return tile

    def flux_tile(v):
        return flux[pl.ds(pl.multiple_of(v * 8, 8), 8), :]

    own, own_flux, mate = pick_nodes(
        [
            ([plane_tile(HALO + 2 * core), flux_tile], surf_ref[pl.ds(2 + core, 1)][0]),
            ([plane_tile(HALO + 2 - 2 * core)], surf_ref[pl.ds(3 - core, 1)][0]),
        ]
    )
    is_first = core == 0
    keep[pl.ds(4 * ROWS, 8), :] = jnp.concatenate(
        [jnp.where(is_first, own, mate), jnp.where(is_first, mate, own)], axis=0
    )
    if full:
        block = jnp.concatenate([own, own_flux], axis=0)
    else:
        block = flts[3:4, :] * own + flts[4:5, :] * own_flux
    export[...] = jnp.broadcast_to(block[None], export.shape)


def pack_kernel(fields, surface, payload):
    for i in range(4):
        rows = fields[i].reshape(2 * ROWS, 128)
        for p in range(2):
            for lane in range(8):
                start = p * ROWS + 16 * lane
                payload[pl.ds(256 * i + p * ROWS + lane, 16, stride=8), :] = rows[start : start + 16]
    cells = surface[...].reshape(4, 128)
    row = (cells >> 7) & (ROWS - 1)
    kept = ((row & 15) << 3) | (row >> 4)
    cells = ((cells & ~(127 << 7)) | (kept << 7)).astype(F32)
    payload[pl.ds(1024, 8), :] = jnp.concatenate([cells, cells], axis=0)


def prepare_kernel(kinds, partners, counts, centres, maps, ints, flts, place, turned):
    group = lax.axis_index("grp")
    me = lax.axis_index("sub")
    subs = counts.shape[1]
    nodes = subs * 512
    live = counts[0, me]
    kind = kinds[group]
    at = centres[...]
    anchor = at[0:1, 0:1]
    apart = ((at - anchor + nodes // 2) & (nodes - 1)) - nodes // 2
    apart = jnp.where(iota(at.shape, 0) < live, apart, 0)
    lowest = jnp.min(apart.astype(F32)).astype(jnp.int32)
    start = (jnp.max(anchor.astype(F32)).astype(jnp.int32) + lowest) & (nodes - 1)
    first = start >> 9
    place[...] = jnp.where(iota(at.shape, 0) < live, (at - first * 512) & (nodes - 1), -1)
    ints[...] = jnp.full(ints.shape, partners[group] * subs + first, jnp.int32)
    is_gas = kind == 0
    for row, (gas, solid) in enumerate(((0.5, 0.25), (-0.25, 0.25), (1.0, 0.0), (0.25, 0.5), (0.25, -0.25))):
        flts[pl.ds(row, 1), :] = jnp.full((1, 128), jnp.where(is_gas, gas, solid), F32)
    for s in range(maps.shape[0]):
        turned[s] = maps[s].T


def far_kernel(mate, far):
    skip = jnp.where((lax.axis_index("sub") & 1) == 0, 0, ROWS)
    far[pl.ds(0, 2 * ROWS), :] = mate[pl.ds(0, 2 * ROWS), :]
    for which in range(3):
        start = pl.multiple_of(256 * (which + 1) + skip, ROWS)
        far[pl.ds((2 + which) * ROWS, ROWS), :] = mate[pl.ds(start, ROWS), :]
    far[pl.ds(5 * ROWS, 8), :] = mate[pl.ds(1024, 8), :]


def first_kernel(flts, own, mate, near, near_other, far, far_other,
                 keep, export, coef, surf, cur, nxt, flux):
    first = (lax.axis_index("sub") & 1) == 0
    gas = flts[2:3, :]

    def pick(one, other, start, size):
        x = one[pl.ds(start, size), :]
        y = other[pl.ds(start, size), :]
        return jnp.where(first, x, y), jnp.where(first, y, x)

    pairs = ((far, far_other, 5 * ROWS, (0, 5)), (near, near_other, 1024, (1, 4)), (own, mate, 1024, (2, 3)))
    for one, other, tail, blocks in pairs:
        both = pick(one, other, 0, 2 * ROWS)
        cells = pick(one, other, tail, 8)
        for side, block in enumerate(blocks):
            cur[2 * block] = both[side][:ROWS]
            cur[2 * block + 1] = both[side][ROWS:]
            surf[block] = cells[side][:4].astype(jnp.int32)

    def store(one, other, starts, planes):
        got = [pick(one, other, start, ROWS) for start in starts]
        for side, plane in enumerate(planes):
            conduct, velocity, heat = (g[side] for g in got)
            coef[0, plane - 1] = conduct
            flow = conduct + gas * velocity
            coef[1, plane - 1] = flow
            coef[3, plane - 1] = 1.0 - 5.0 * conduct - flow
            coef[2, plane - 1] = (0.5 * gas) * heat

    for half in range(2):
        starts = [256 * (w + 1) + half * ROWS for w in range(3)]
        store(own, mate, starts, (4 + half, 6 + half))
        store(near, near_other, starts, (2 + half, 8 + half))
    store(far, far_other, [(2 + w) * ROWS for w in range(3)], (1, 10))
    run_steps(cur, nxt, coef)
    finish(flts, cur, coef, surf, flux, keep, export, False)


def middle_kernel(flts, parts, own, beside, other, surf, coef, keep, export,
                  cur, nxt, flux, *, full):
    first = (lax.axis_index("sub") & 1) == 0
    total = sum_parts(parts)

    def sides(start, size):
        near = beside[pl.ds(start, size), :]
        far = other[pl.ds(start, size), :]
        return jnp.where(first, near, far), own[pl.ds(start, size), :], jnp.where(first, far, near)

    temps = sides(4 * ROWS, 8)
    incs = [total[8 * side : 8 * side + 8] - flts[0:1, :] * temps[side] for side in range(3)]
    for half in range(2):
        planes = sides(2 * half * ROWS, 2 * ROWS)
        for side in range(3):
            block = 2 * side + half
            out = planes[side] + scatter_block(surf[block], incs[side][4 * half : 4 * half + 4])
            cur[2 * block] = out[:ROWS]
            cur[2 * block + 1] = out[ROWS:]
    run_steps(cur, nxt, coef)
    finish(flts, cur, coef, surf, flux, keep, export, full)


def sum_parts(parts):
    lanes = [parts[i] for i in range(4)]
    for i in range(4, parts.shape[0]):
        lanes[i % 4] = lanes[i % 4] + parts[i]
    return (lanes[0] + lanes[1]) + (lanes[2] + lanes[3])


def last_kernel(flts, parts, own, surf, field, interface, work):
    core = lax.axis_index("sub") & 1
    total = sum_parts(parts)
    interface[...] = total.reshape(2, 512)
    temps = own[pl.ds(4 * ROWS, 8), :]
    temps = jnp.where(core == 0, temps[:4], temps[4:])
    inc = flts[0:1, :] * (total[:4] - temps) + flts[1:2, :] * total[4:]
    add = scatter_block(surf[pl.ds(2 + core, 1)][0], inc)
    start = pl.multiple_of(core * 2 * ROWS, 2 * ROWS)
    work[...] = own[pl.ds(start, 2 * ROWS), :] + add
    rows = [work[pl.ds(p * ROWS + lane, 16, stride=8), :] for p in range(2) for lane in range(8)]
    field[...] = jnp.concatenate(rows, axis=0).reshape(2, 128 * ROWS)


def patch_kernel(ints, source, place, targets, maps, out, *, final):
    slots = place.shape[0]
    subs = out.shape[0]
    parts = 2 if final else 1
    lanes = [place[pl.ds(8 * w, 8), :] & 127 for w in range(slots // 8)]
    rows = [place[pl.ds(8 * w, 8), :] >> 7 for w in range(slots // 8)]
    vals = [[jnp.zeros((8, 128), F32) for _ in rows] for _ in range(parts)]
    at = jnp.max(ints[0:1, :].astype(F32)).astype(jnp.int32)
    for i in range(3):
        tile = source[(at & -subs) + ((at + i) & (subs - 1))]
        for q in range(parts):
            for j in range(4):
                line = jnp.broadcast_to(tile[4 * q + j : 4 * q + j + 1], (8, 128))
                for w in range(slots // 8):
                    got = jnp.take_along_axis(line, lanes[w], axis=1, mode="promise_in_bounds")
                    vals[q][w] = jnp.where(rows[w] == 4 * i + j, got, vals[q][w])
    columns = []
    for q in range(parts):
        full = jnp.concatenate(vals[q] + [jnp.zeros((128 - slots, 128), F32)], axis=0)
        columns.append(full.T)
    left, right = [], [[] for _ in range(parts)]
    for s in range(slots):
        aim = targets[s : s + 1, :]
        left.append(one_hot(aim >> 7, 128))
        table = maps[s]
        for q in range(parts):
            value = jnp.sum(table * columns[q][:, s : s + 1], axis=0, keepdims=True)
            right[q].append(spread(aim & 127, value))
    sums = [product(left, right[q]) for q in range(parts)]
    chips = out.shape[0] // 2
    for c in range(chips):
        if final:
            for k in range(2):
                r = 2 * c + k
                out[r] = jnp.concatenate([s[4 * r : 4 * r + 4] for s in sums], axis=0)
        else:
            for side in range(3):
                n = c + side - 1
                piece = sums[0][8 * n : 8 * n + 8] if 0 <= n < chips else jnp.zeros((8, 128), F32)
                for k in range(2):
                    out[2 * c + k, pl.ds(8 * side, 8), :] = piece


def call(kernel, ins, outs, scratch=()):
    where = {"s": SMEM, "v": VMEM}
    return pl.pallas_call(
        kernel,
        out_shape=[jax.ShapeDtypeStruct(s, d) for s, d, _ in outs],
        in_specs=[pl.BlockSpec(memory_space=where[i]) for i in ins],
        out_specs=[pl.BlockSpec(memory_space=where[o]) for _, _, o in outs],
        scratch_shapes=[pltpu.VMEM(s, F32) for s in scratch],
        compiler_params=pltpu.CompilerParams(vmem_limit_bytes=16 * 1024 * 1024),
    )


def local(
    initial_field,
    conduct,
    velocity,
    heat_release,
    group_kind,
    partner,
    surface_cell,
    patch_count,
    patch_centres,
    patch_targets,
    patch_maps,
):
    subs = lax.axis_size("sub")
    groups = lax.axis_size("grp")
    block = surface_cell.shape[1]
    slots = patch_maps.shape[1]
    planes, cells = initial_field.shape[1:]

    fields = jnp.concatenate([initial_field, conduct, velocity, heat_release], axis=0)
    (payload,) = call(pack_kernel, "vv", [((1032, 128), F32, "v")])(fields, surface_cell)
    swap = [(i, i ^ 1) for i in range(subs)]
    cross = [(i, i + 1 if i % 2 else i - 1) for i in range(1, subs - 1)]
    near = lax.ppermute(payload, "sub", cross)
    mate = lax.ppermute(payload, "sub", swap)
    (far,) = call(far_kernel, "v", [((5 * ROWS + 8, 128), F32, "v")])(mate)
    far = lax.ppermute(far, "sub", cross)
    ints, flts, place, turned = call(
        prepare_kernel,
        "sssvv",
        [
            ((8, 128), jnp.int32, "v"),
            ((8, 128), F32, "v"),
            ((slots, 128), jnp.int32, "v"),
            ((slots, 128, 128), F32, "v"),
        ],
    )(group_kind, partner, patch_count, patch_centres[0], patch_maps[0])
    targets = patch_targets[0]
    near_other = lax.ppermute(near, "sub", swap)
    far_other = lax.ppermute(far, "sub", swap)

    keep_out = ((4 * ROWS + 8, 128), F32, "v")
    half_out = ((groups * subs, 4, 128), F32, "v")
    full_out = ((groups * subs, 8, 128), F32, "v")
    coef_shape = (4, WIDE - 2, ROWS, 128)
    work = [(WIDE, ROWS, 128), (WIDE, ROWS, 128), (2 * ROWS, 128)]
    keep, send, coef, surf = call(
        first_kernel,
        "vvvvvvv",
        [keep_out, half_out, (coef_shape, F32, "v"), ((6, 4, 128), jnp.int32, "v")],
        work,
    )(flts, payload, mate, near, near_other, far, far_other)
    for iteration in range(COUPLE):
        final = iteration == COUPLE - 1
        if not final:
            beside = lax.ppermute(keep, "sub", cross)
        source = lax.all_to_all(send, ("grp", "sub"), 0, 0, tiled=True)
        if not final:
            source, beside = lax.optimization_barrier((source, beside))
            other = lax.ppermute(beside, "sub", swap)
        (parts,) = call(
            functools.partial(patch_kernel, final=final),
            "vvvvv",
            [((subs, 8 if final else 24, 128), F32, "v")],
        )(ints, source, place, targets, turned)
        if not final:
            parts, other = lax.optimization_barrier((parts, other))
        parts = lax.all_to_all(parts, "sub", 0, 0, tiled=True)
        if final:
            field, interface = call(
                last_kernel,
                "vvvv",
                [((planes, cells), F32, "v"), ((2, block), F32, "v")],
                [(2 * ROWS, 128)],
            )(flts, parts, keep, surf)
        else:
            full = iteration == COUPLE - 2
            keep, send = call(
                functools.partial(middle_kernel, full=full),
                "vvvvvvv",
                [keep_out, full_out if full else half_out],
                work,
            )(flts, parts, keep, beside, other, surf, coef)
    return field[None], interface[None]


def solution(mesh):
    placed = (
        P("grp", "sub", None),
        P("grp", "sub", None),
        P("grp", "sub", None),
        P("grp", "sub", None),
        P(),
        P(),
        P("grp", "sub"),
        P("grp", None),
        P("grp", "sub", None),
        P("grp", "sub", None),
        P("grp", "sub", None, None),
    )
    return jax.shard_map(
        local,
        mesh=mesh,
        in_specs=placed,
        out_specs=(P("grp", "sub", None), P("grp", None, "sub")),
        check_vma=False,
    )
```

```python
import functools

import jax
import jax.numpy as jnp
from jax import lax
from jax.experimental import pallas as pl
from jax.experimental.pallas import tpu as pltpu
from jax.sharding import PartitionSpec as P


STEPS = 4
COUPLE = 4
ROWS = 128
HALO = 4
WIDE = 12
F32 = jnp.float32
BF16 = jnp.bfloat16
VMEM = pltpu.VMEM
SMEM = pltpu.SMEM


def iota(shape, dim):
    return lax.broadcasted_iota(jnp.int32, shape, dim)


def in_plane(x):
    above = jnp.concatenate([pltpu.roll(x[ROWS - 8 :], 1, 0), x[: ROWS - 8]], axis=0)
    below = jnp.concatenate([x[8:], pltpu.roll(x[:8], 7, 0)], axis=0)
    return (above + below) + (pltpu.roll(x, 1, 1) + pltpu.roll(x, 127, 1))


def run_steps(cur, nxt, coef):
    bufs = (cur, nxt)
    for step in range(STEPS):
        src, dst = bufs[step % 2], bufs[(step + 1) % 2]

        def body(p, carry, src=src, dst=dst):
            x = src[p]
            near = src[p + 1] + in_plane(x)
            dst[p] = (coef[3, p - 1] * x + coef[0, p - 1] * near) + (
                coef[1, p - 1] * src[p - 1] + coef[2, p - 1] * (1.0 + jnp.tanh(x))
            )
            return carry

        lax.fori_loop(step + 1, WIDE - 1 - step, body, 0, unroll=True)


def pick_nodes(jobs):
    keys = []
    for _, surf in jobs:
        lanes = [jnp.broadcast_to(surf[g : g + 1] & 127, (8, 128)) for g in range(4)]
        rows = [jnp.broadcast_to(surf[g : g + 1] >> 7, (8, 128)) - iota((8, 128), 0) for g in range(4)]
        keys.append((lanes, rows))

    def body(v, acc):
        out = []
        for (tables, _), (lanes, rows) in zip(jobs, keys):
            hits = [rows[g] == 8 * v for g in range(4)]
            for table in tables:
                tile = table(v)
                for g in range(4):
                    got = jnp.take_along_axis(tile, lanes[g], axis=1, mode="promise_in_bounds")
                    out.append(jnp.where(hits[g], got, acc[len(out)]))
        return tuple(out)

    total = sum(len(tables) for tables, _ in jobs)
    acc = lax.fori_loop(0, 32, body, tuple(jnp.zeros((8, 128), F32) for _ in range(4 * total)), unroll=8)
    return [
        jnp.concatenate([jnp.sum(acc[4 * t + g], axis=0, keepdims=True) for g in range(4)], axis=0)
        for t in range(total)
    ]


def halves(x):
    high = x.astype(BF16)
    return high, (x - high.astype(F32)).astype(BF16)


def rows_at(index, count):
    return iota((count, 128), 0).astype(F32).astype(BF16) == index.astype(F32).astype(BF16)


def one_hot(index, count):
    return jnp.where(rows_at(index, count), jnp.bfloat16(1), jnp.bfloat16(0))


def spread(index, value):
    hit = rows_at(index, 128)
    return jnp.concatenate([jnp.where(hit, part, jnp.bfloat16(0)) for part in halves(value)], axis=0)


def product(left, right):
    out = lax.dot_general(
        jnp.concatenate(left, axis=1),
        jnp.concatenate(right, axis=1),
        (((1,), (1,)), ((), ())),
        preferred_element_type=F32,
    )
    return out[:, :128] + out[:, 128:]


def scatter_block(surf, inc):
    groups = [slice(g, g + 1) for g in range(4)]
    return product(
        [one_hot(surf[g] >> 7, 256) for g in groups], [spread(surf[g] & 127, inc[g]) for g in groups]
    )


def finish(flts, cur, coef, surf_ref, flux, keep, export, full):
    core = lax.axis_index("sub") & 1
    for p in range(4):
        keep[pl.ds(p * ROWS, ROWS), :] = cur[HALO + p]
    for p in range(2):
        x = cur[HALO + 2 * core + p]
        flux[pl.ds(p * ROWS, ROWS), :] = coef[0, HALO - 1 + 2 * core + p] * (4.0 * x - in_plane(x))

    def plane_tile(first):
        def tile(v):
            return cur[first + v // 16, pl.ds(pl.multiple_of((v % 16) * 8, 8), 8), :]

        return tile

    def flux_tile(v):
        return flux[pl.ds(pl.multiple_of(v * 8, 8), 8), :]

    own, own_flux, mate = pick_nodes(
        [
            ([plane_tile(HALO + 2 * core), flux_tile], surf_ref[pl.ds(2 + core, 1)][0]),
            ([plane_tile(HALO + 2 - 2 * core)], surf_ref[pl.ds(3 - core, 1)][0]),
        ]
    )
    is_first = core == 0
    keep[pl.ds(4 * ROWS, 8), :] = jnp.concatenate(
        [jnp.where(is_first, own, mate), jnp.where(is_first, mate, own)], axis=0
    )
    if full:
        block = jnp.concatenate([own, own_flux], axis=0)
    else:
        block = flts[3:4, :] * own + flts[4:5, :] * own_flux
    export[...] = jnp.broadcast_to(block[None], export.shape)


def pack_kernel(fields, surface, payload):
    for i in range(4):
        rows = fields[i].reshape(2 * ROWS, 128)
        for p in range(2):
            for lane in range(8):
                start = p * ROWS + 16 * lane
                payload[pl.ds(256 * i + p * ROWS + lane, 16, stride=8), :] = rows[start : start + 16]
    cells = surface[...].reshape(4, 128)
    row = (cells >> 7) & (ROWS - 1)
    kept = ((row & 15) << 3) | (row >> 4)
    cells = ((cells & ~(127 << 7)) | (kept << 7)).astype(F32)
    payload[pl.ds(1024, 8), :] = jnp.concatenate([cells, cells], axis=0)


def prepare_kernel(kinds, partners, counts, centres, maps, ints, flts, place, turned):
    group = lax.axis_index("grp")
    me = lax.axis_index("sub")
    subs = counts.shape[1]
    nodes = subs * 512
    live = counts[0, me]
    kind = kinds[group]
    at = centres[...]
    anchor = at[0:1, 0:1]
    apart = ((at - anchor + nodes // 2) & (nodes - 1)) - nodes // 2
    apart = jnp.where(iota(at.shape, 0) < live, apart, 0)
    lowest = jnp.min(apart.astype(F32)).astype(jnp.int32)
    start = (jnp.max(anchor.astype(F32)).astype(jnp.int32) + lowest) & (nodes - 1)
    first = start >> 9
    place[...] = jnp.where(iota(at.shape, 0) < live, (at - first * 512) & (nodes - 1), -1)
    ints[...] = jnp.full(ints.shape, partners[group] * subs + first, jnp.int32)
    is_gas = kind == 0
    for row, (gas, solid) in enumerate(((0.5, 0.25), (-0.25, 0.25), (1.0, 0.0), (0.25, 0.5), (0.25, -0.25))):
        flts[pl.ds(row, 1), :] = jnp.full((1, 128), jnp.where(is_gas, gas, solid), F32)
    for s in range(maps.shape[0]):
        turned[pl.ds(128 * s, 128), :] = jnp.concatenate(halves(maps[s].T), axis=1)


def far_kernel(mate, far):
    skip = jnp.where((lax.axis_index("sub") & 1) == 0, 0, ROWS)
    far[pl.ds(0, 2 * ROWS), :] = mate[pl.ds(0, 2 * ROWS), :]
    for which in range(3):
        start = pl.multiple_of(256 * (which + 1) + skip, ROWS)
        far[pl.ds((2 + which) * ROWS, ROWS), :] = mate[pl.ds(start, ROWS), :]
    far[pl.ds(5 * ROWS, 8), :] = mate[pl.ds(1024, 8), :]


def first_kernel(flts, own, mate, near, near_other, far, far_other,
                 keep, export, coef, surf, cur, nxt, flux):
    first = (lax.axis_index("sub") & 1) == 0
    gas = flts[2:3, :]

    def pick(one, other, start, size):
        x = one[pl.ds(start, size), :]
        y = other[pl.ds(start, size), :]
        return jnp.where(first, x, y), jnp.where(first, y, x)

    pairs = ((far, far_other, 5 * ROWS, (0, 5)), (near, near_other, 1024, (1, 4)), (own, mate, 1024, (2, 3)))
    for one, other, tail, blocks in pairs:
        both = pick(one, other, 0, 2 * ROWS)
        cells = pick(one, other, tail, 8)
        for side, block in enumerate(blocks):
            cur[2 * block] = both[side][:ROWS]
            cur[2 * block + 1] = both[side][ROWS:]
            surf[block] = cells[side][:4].astype(jnp.int32)

    def store(one, other, starts, planes):
        got = [pick(one, other, start, ROWS) for start in starts]
        for side, plane in enumerate(planes):
            conduct, velocity, heat = (g[side] for g in got)
            coef[0, plane - 1] = conduct
            flow = conduct + gas * velocity
            coef[1, plane - 1] = flow
            coef[3, plane - 1] = 1.0 - 5.0 * conduct - flow
            coef[2, plane - 1] = (0.5 * gas) * heat

    for half in range(2):
        starts = [256 * (w + 1) + half * ROWS for w in range(3)]
        store(own, mate, starts, (4 + half, 6 + half))
        store(near, near_other, starts, (2 + half, 8 + half))
    store(far, far_other, [(2 + w) * ROWS for w in range(3)], (1, 10))
    run_steps(cur, nxt, coef)
    finish(flts, cur, coef, surf, flux, keep, export, False)


def middle_kernel(flts, parts, own, beside, other, surf, coef, keep, export,
                  cur, nxt, flux, *, full):
    first = (lax.axis_index("sub") & 1) == 0
    total = sum_parts(parts)

    def sides(start, size):
        near = beside[pl.ds(start, size), :]
        far = other[pl.ds(start, size), :]
        return jnp.where(first, near, far), own[pl.ds(start, size), :], jnp.where(first, far, near)

    temps = sides(4 * ROWS, 8)
    incs = [total[8 * side : 8 * side + 8] - flts[0:1, :] * temps[side] for side in range(3)]
    for half in range(2):
        planes = sides(2 * half * ROWS, 2 * ROWS)
        for side in range(3):
            block = 2 * side + half
            out = planes[side] + scatter_block(surf[block], incs[side][4 * half : 4 * half + 4])
            cur[2 * block] = out[:ROWS]
            cur[2 * block + 1] = out[ROWS:]
    run_steps(cur, nxt, coef)
    finish(flts, cur, coef, surf, flux, keep, export, full)


def sum_parts(parts):
    lanes = [parts[i] for i in range(4)]
    for i in range(4, parts.shape[0]):
        lanes[i % 4] = lanes[i % 4] + parts[i]
    return (lanes[0] + lanes[1]) + (lanes[2] + lanes[3])


def last_kernel(flts, parts, own, surf, field, interface, work):
    core = lax.axis_index("sub") & 1
    total = sum_parts(parts)
    interface[...] = total.reshape(2, 512)
    temps = own[pl.ds(4 * ROWS, 8), :]
    temps = jnp.where(core == 0, temps[:4], temps[4:])
    inc = flts[0:1, :] * (total[:4] - temps) + flts[1:2, :] * total[4:]
    add = scatter_block(surf[pl.ds(2 + core, 1)][0], inc)
    start = pl.multiple_of(core * 2 * ROWS, 2 * ROWS)
    work[...] = own[pl.ds(start, 2 * ROWS), :] + add
    rows = [work[pl.ds(p * ROWS + lane, 16, stride=8), :] for p in range(2) for lane in range(8)]
    field[...] = jnp.concatenate(rows, axis=0).reshape(2, 128 * ROWS)


def patch_kernel(ints, source, place, targets, maps, out, *, final):
    slots = place.shape[0]
    subs = out.shape[0]
    parts = 2 if final else 1
    lanes = [place[pl.ds(8 * w, 8), :] & 127 for w in range(slots // 8)]
    rows = [place[pl.ds(8 * w, 8), :] >> 7 for w in range(slots // 8)]
    vals = [[jnp.zeros((8, 128), F32) for _ in rows] for _ in range(parts)]
    at = jnp.max(ints[0:1, :].astype(F32)).astype(jnp.int32)
    for i in range(3):
        tile = source[(at & -subs) + ((at + i) & (subs - 1))]
        for q in range(parts):
            for j in range(4):
                line = jnp.broadcast_to(tile[4 * q + j : 4 * q + j + 1], (8, 128))
                for w in range(slots // 8):
                    got = jnp.take_along_axis(line, lanes[w], axis=1, mode="promise_in_bounds")
                    vals[q][w] = jnp.where(rows[w] == 4 * i + j, got, vals[q][w])
    heads = []
    for q in range(parts):
        heads.extend(halves(jnp.concatenate(vals[q] + [jnp.zeros((32 - slots, 128), F32)], axis=0)))
    head = jnp.concatenate(heads, axis=0)
    blocks = []
    for s in range(slots):
        mine = iota((32, 128), 0).astype(F32).astype(BF16) == jnp.bfloat16(s)
        blocks.append(jnp.where(jnp.concatenate([mine] * (2 * parts), axis=0), head, jnp.bfloat16(0)))
    out_rows = jnp.dot(jnp.concatenate(blocks, axis=1), maps[...], preferred_element_type=F32)
    out_rows = out_rows[:, :128] + out_rows[:, 128:]
    values = [out_rows[64 * q : 64 * q + 32] + out_rows[64 * q + 32 : 64 * q + 64] for q in range(parts)]
    left, right = [], [[] for _ in range(parts)]
    for s in range(slots):
        aim = targets[s : s + 1, :]
        left.append(one_hot(aim >> 7, 128))
        for q in range(parts):
            right[q].append(spread(aim & 127, values[q][s : s + 1]))
    sums = [product(left, right[q]) for q in range(parts)]
    chips = out.shape[0] // 2
    for c in range(chips):
        if final:
            for k in range(2):
                r = 2 * c + k
                out[r] = jnp.concatenate([s[4 * r : 4 * r + 4] for s in sums], axis=0)
        else:
            for side in range(3):
                n = c + side - 1
                piece = sums[0][8 * n : 8 * n + 8] if 0 <= n < chips else jnp.zeros((8, 128), F32)
                for k in range(2):
                    out[2 * c + k, pl.ds(8 * side, 8), :] = piece


def call(kernel, ins, outs, scratch=()):
    where = {"s": SMEM, "v": VMEM}
    return pl.pallas_call(
        kernel,
        out_shape=[jax.ShapeDtypeStruct(s, d) for s, d, _ in outs],
        in_specs=[pl.BlockSpec(memory_space=where[i]) for i in ins],
        out_specs=[pl.BlockSpec(memory_space=where[o]) for _, _, o in outs],
        scratch_shapes=[pltpu.VMEM(s, F32) for s in scratch],
        compiler_params=pltpu.CompilerParams(vmem_limit_bytes=16 * 1024 * 1024),
    )


def local(
    initial_field,
    conduct,
    velocity,
    heat_release,
    group_kind,
    partner,
    surface_cell,
    patch_count,
    patch_centres,
    patch_targets,
    patch_maps,
):
    subs = lax.axis_size("sub")
    groups = lax.axis_size("grp")
    block = surface_cell.shape[1]
    slots = patch_maps.shape[1]
    planes, cells = initial_field.shape[1:]

    fields = jnp.concatenate([initial_field, conduct, velocity, heat_release], axis=0)
    (payload,) = call(pack_kernel, "vv", [((1032, 128), F32, "v")])(fields, surface_cell)
    swap = [(i, i ^ 1) for i in range(subs)]
    cross = [(i, i + 1 if i % 2 else i - 1) for i in range(1, subs - 1)]
    near = lax.ppermute(payload, "sub", cross)
    mate = lax.ppermute(payload, "sub", swap)
    (far,) = call(far_kernel, "v", [((5 * ROWS + 8, 128), F32, "v")])(mate)
    far = lax.ppermute(far, "sub", cross)
    ints, flts, place, turned = call(
        prepare_kernel,
        "sssvv",
        [
            ((8, 128), jnp.int32, "v"),
            ((8, 128), F32, "v"),
            ((slots, 128), jnp.int32, "v"),
            ((slots * 128, 256), BF16, "v"),
        ],
    )(group_kind, partner, patch_count, patch_centres[0], patch_maps[0])
    targets = patch_targets[0]
    near_other = lax.ppermute(near, "sub", swap)
    far_other = lax.ppermute(far, "sub", swap)

    keep_out = ((4 * ROWS + 8, 128), F32, "v")
    half_out = ((groups * subs, 4, 128), F32, "v")
    full_out = ((groups * subs, 8, 128), F32, "v")
    coef_shape = (4, WIDE - 2, ROWS, 128)
    work = [(WIDE, ROWS, 128), (WIDE, ROWS, 128), (2 * ROWS, 128)]
    keep, send, coef, surf = call(
        first_kernel,
        "vvvvvvv",
        [keep_out, half_out, (coef_shape, F32, "v"), ((6, 4, 128), jnp.int32, "v")],
        work,
    )(flts, payload, mate, near, near_other, far, far_other)
    for iteration in range(COUPLE):
        final = iteration == COUPLE - 1
        if not final:
            beside = lax.ppermute(keep, "sub", cross)
        source = lax.all_to_all(send, ("grp", "sub"), 0, 0, tiled=True)
        if not final:
            source, beside = lax.optimization_barrier((source, beside))
            other = lax.ppermute(beside, "sub", swap)
        (parts,) = call(
            functools.partial(patch_kernel, final=final),
            "vvvvv",
            [((subs, 8 if final else 24, 128), F32, "v")],
        )(ints, source, place, targets, turned)
        if not final:
            parts, other = lax.optimization_barrier((parts, other))
        parts = lax.all_to_all(parts, "sub", 0, 0, tiled=True)
        if final:
            field, interface = call(
                last_kernel,
                "vvvv",
                [((planes, cells), F32, "v"), ((2, block), F32, "v")],
                [(2 * ROWS, 128)],
            )(flts, parts, keep, surf)
        else:
            full = iteration == COUPLE - 2
            keep, send = call(
                functools.partial(middle_kernel, full=full),
                "vvvvvvv",
                [keep_out, full_out if full else half_out],
                work,
            )(flts, parts, keep, beside, other, surf, coef)
    return field[None], interface[None]


def solution(mesh):
    placed = (
        P("grp", "sub", None),
        P("grp", "sub", None),
        P("grp", "sub", None),
        P("grp", "sub", None),
        P(),
        P(),
        P("grp", "sub"),
        P("grp", None),
        P("grp", "sub", None),
        P("grp", "sub", None),
        P("grp", "sub", None, None),
    )
    return jax.shard_map(
        local,
        mesh=mesh,
        in_specs=placed,
        out_specs=(P("grp", "sub", None), P("grp", None, "sub")),
        check_vma=False,
    )
```

```python
import functools

import jax
import jax.numpy as jnp
from jax import lax
from jax.experimental import pallas as pl
from jax.experimental.pallas import tpu as pltpu
from jax.sharding import PartitionSpec as P


STEPS = 4
COUPLE = 4
ROWS = 128
PIECE = 16
HALO = 4
WIDE = 12
F32 = jnp.float32
BF16 = jnp.bfloat16
VMEM = pltpu.VMEM
SMEM = pltpu.SMEM


def iota(shape, dim):
    return lax.broadcasted_iota(jnp.int32, shape, dim)


def in_plane(x):
    above = jnp.concatenate([pltpu.roll(x[ROWS - 8 :], 1, 0), x[: ROWS - 8]], axis=0)
    below = jnp.concatenate([x[8:], pltpu.roll(x[:8], 7, 0)], axis=0)
    return (above + below) + (pltpu.roll(x, 1, 1) + pltpu.roll(x, 127, 1))


def run_steps(cur, nxt, coef):
    bufs = (cur, nxt)
    for step in range(STEPS):
        src, dst = bufs[step % 2], bufs[(step + 1) % 2]

        def body(p, carry, src=src, dst=dst):
            for low in range(0, ROWS, PIECE):
                high = low + PIECE
                rows = pl.ds(low, PIECE)
                if low:
                    before = src[p, pl.ds(low - 8, 8)]
                else:
                    before = pltpu.roll(src[p, pl.ds(ROWS - 8, 8)], 1, 0)
                if high < ROWS:
                    after = src[p, pl.ds(high, 8)]
                else:
                    after = pltpu.roll(src[p, pl.ds(0, 8)], 7, 0)
                x = src[p, rows]
                beside = jnp.concatenate([before, x[:-8]], axis=0) + jnp.concatenate([x[8:], after], axis=0)
                beside = beside + (pltpu.roll(x, 1, 1) + pltpu.roll(x, 127, 1))
                dst[p, rows] = (coef[3, p - 1, rows] * x + coef[0, p - 1, rows] * (src[p + 1, rows] + beside)) + (
                    coef[1, p - 1, rows] * src[p - 1, rows] + coef[2, p - 1, rows] * (1.0 + jnp.tanh(x))
                )
            return carry

        lax.fori_loop(step + 1, WIDE - 1 - step, body, 0, unroll=True)


def pick_nodes(jobs):
    keys = []
    for _, surf in jobs:
        lanes = [jnp.broadcast_to(surf[g : g + 1] & 127, (8, 128)) for g in range(4)]
        rows = [jnp.broadcast_to(surf[g : g + 1] >> 7, (8, 128)) - iota((8, 128), 0) for g in range(4)]
        keys.append((lanes, rows))

    def body(v, acc):
        out = []
        for (tables, _), (lanes, rows) in zip(jobs, keys):
            hits = [rows[g] == 8 * v for g in range(4)]
            for table in tables:
                tile = table(v)
                for g in range(4):
                    got = jnp.take_along_axis(tile, lanes[g], axis=1, mode="promise_in_bounds")
                    out.append(jnp.where(hits[g], got, acc[len(out)]))
        return tuple(out)

    total = sum(len(tables) for tables, _ in jobs)
    acc = lax.fori_loop(0, 32, body, tuple(jnp.zeros((8, 128), F32) for _ in range(4 * total)), unroll=8)
    return [
        jnp.concatenate([jnp.sum(acc[4 * t + g], axis=0, keepdims=True) for g in range(4)], axis=0)
        for t in range(total)
    ]


def halves(x):
    high = x.astype(BF16)
    return high, (x - high.astype(F32)).astype(BF16)


def rows_at(index, count):
    return iota((count, 128), 0).astype(F32).astype(BF16) == index.astype(F32).astype(BF16)


def one_hot(index, count):
    return jnp.where(rows_at(index, count), jnp.bfloat16(1), jnp.bfloat16(0))


def spread(index, value):
    hit = rows_at(index, 128)
    return jnp.concatenate([jnp.where(hit, part, jnp.bfloat16(0)) for part in halves(value)], axis=0)


def product(left, right):
    out = lax.dot_general(
        jnp.concatenate(left, axis=1),
        jnp.concatenate(right, axis=1),
        (((1,), (1,)), ((), ())),
        preferred_element_type=F32,
    )
    return out[:, :128] + out[:, 128:]


def scatter_block(surf, inc):
    groups = [slice(g, g + 1) for g in range(4)]
    return product(
        [one_hot(surf[g] >> 7, 256) for g in groups], [spread(surf[g] & 127, inc[g]) for g in groups]
    )


def finish(flts, cur, coef, surf_ref, flux, keep, export, full):
    core = lax.axis_index("sub") & 1
    for p in range(4):
        keep[pl.ds(p * ROWS, ROWS), :] = cur[HALO + p]
    for p in range(2):
        x = cur[HALO + 2 * core + p]
        flux[pl.ds(p * ROWS, ROWS), :] = coef[0, HALO - 1 + 2 * core + p] * (4.0 * x - in_plane(x))

    def plane_tile(first):
        def tile(v):
            return cur[first + v // 16, pl.ds(pl.multiple_of((v % 16) * 8, 8), 8), :]

        return tile

    def flux_tile(v):
        return flux[pl.ds(pl.multiple_of(v * 8, 8), 8), :]

    own, own_flux, mate = pick_nodes(
        [
            ([plane_tile(HALO + 2 * core), flux_tile], surf_ref[pl.ds(2 + core, 1)][0]),
            ([plane_tile(HALO + 2 - 2 * core)], surf_ref[pl.ds(3 - core, 1)][0]),
        ]
    )
    is_first = core == 0
    keep[pl.ds(4 * ROWS, 8), :] = jnp.concatenate(
        [jnp.where(is_first, own, mate), jnp.where(is_first, mate, own)], axis=0
    )
    if full:
        block = jnp.concatenate([own, own_flux], axis=0)
    else:
        block = flts[3:4, :] * own + flts[4:5, :] * own_flux
    export[...] = jnp.broadcast_to(block[None], export.shape)


def pack_kernel(fields, surface, payload):
    for i in range(4):
        rows = fields[i].reshape(2 * ROWS, 128)
        for p in range(2):
            for lane in range(8):
                start = p * ROWS + 16 * lane
                payload[pl.ds(256 * i + p * ROWS + lane, 16, stride=8), :] = rows[start : start + 16]
    cells = surface[...].reshape(4, 128)
    row = (cells >> 7) & (ROWS - 1)
    kept = ((row & 15) << 3) | (row >> 4)
    cells = ((cells & ~(127 << 7)) | (kept << 7)).astype(F32)
    payload[pl.ds(1024, 8), :] = jnp.concatenate([cells, cells], axis=0)


def prepare_kernel(kinds, partners, counts, centres, maps, ints, flts, place, turned):
    group = lax.axis_index("grp")
    me = lax.axis_index("sub")
    subs = counts.shape[1]
    nodes = subs * 512
    live = counts[0, me]
    kind = kinds[group]
    at = centres[...]
    anchor = at[0:1, 0:1]
    apart = ((at - anchor + nodes // 2) & (nodes - 1)) - nodes // 2
    apart = jnp.where(iota(at.shape, 0) < live, apart, 0)
    lowest = jnp.min(apart.astype(F32)).astype(jnp.int32)
    start = (jnp.max(anchor.astype(F32)).astype(jnp.int32) + lowest) & (nodes - 1)
    first = start >> 9
    place[...] = jnp.where(iota(at.shape, 0) < live, (at - first * 512) & (nodes - 1), -1)
    ints[...] = jnp.full(ints.shape, partners[group] * subs + first, jnp.int32)
    is_gas = kind == 0
    for row, (gas, solid) in enumerate(((0.5, 0.25), (-0.25, 0.25), (1.0, 0.0), (0.25, 0.5), (0.25, -0.25))):
        flts[pl.ds(row, 1), :] = jnp.full((1, 128), jnp.where(is_gas, gas, solid), F32)
    for s in range(maps.shape[0]):
        turned[s] = maps[s].T


def far_kernel(mate, far):
    skip = jnp.where((lax.axis_index("sub") & 1) == 0, 0, ROWS)
    far[pl.ds(0, 2 * ROWS), :] = mate[pl.ds(0, 2 * ROWS), :]
    for which in range(3):
        start = pl.multiple_of(256 * (which + 1) + skip, ROWS)
        far[pl.ds((2 + which) * ROWS, ROWS), :] = mate[pl.ds(start, ROWS), :]
    far[pl.ds(5 * ROWS, 8), :] = mate[pl.ds(1024, 8), :]


def first_kernel(flts, own, mate, near, near_other, far, far_other,
                 keep, export, coef, surf, cur, nxt, flux):
    first = (lax.axis_index("sub") & 1) == 0
    gas = flts[2:3, :]

    def pick(one, other, start, size):
        x = one[pl.ds(start, size), :]
        y = other[pl.ds(start, size), :]
        return jnp.where(first, x, y), jnp.where(first, y, x)

    pairs = ((far, far_other, 5 * ROWS, (0, 5)), (near, near_other, 1024, (1, 4)), (own, mate, 1024, (2, 3)))
    for one, other, tail, blocks in pairs:
        both = pick(one, other, 0, 2 * ROWS)
        cells = pick(one, other, tail, 8)
        for side, block in enumerate(blocks):
            cur[2 * block] = both[side][:ROWS]
            cur[2 * block + 1] = both[side][ROWS:]
            surf[block] = cells[side][:4].astype(jnp.int32)

    def store(one, other, starts, planes):
        got = [pick(one, other, start, ROWS) for start in starts]
        for side, plane in enumerate(planes):
            conduct, velocity, heat = (g[side] for g in got)
            coef[0, plane - 1] = conduct
            flow = conduct + gas * velocity
            coef[1, plane - 1] = flow
            coef[3, plane - 1] = 1.0 - 5.0 * conduct - flow
            coef[2, plane - 1] = (0.5 * gas) * heat

    for half in range(2):
        starts = [256 * (w + 1) + half * ROWS for w in range(3)]
        store(own, mate, starts, (4 + half, 6 + half))
        store(near, near_other, starts, (2 + half, 8 + half))
    store(far, far_other, [(2 + w) * ROWS for w in range(3)], (1, 10))
    run_steps(cur, nxt, coef)
    finish(flts, cur, coef, surf, flux, keep, export, False)


def middle_kernel(flts, parts, own, beside, other, surf, coef, keep, export,
                  cur, nxt, flux, *, full):
    first = (lax.axis_index("sub") & 1) == 0
    total = sum_parts(parts)

    def sides(start, size):
        near = beside[pl.ds(start, size), :]
        far = other[pl.ds(start, size), :]
        return jnp.where(first, near, far), own[pl.ds(start, size), :], jnp.where(first, far, near)

    temps = sides(4 * ROWS, 8)
    incs = [total[8 * side : 8 * side + 8] - flts[0:1, :] * temps[side] for side in range(3)]
    for half in range(2):
        planes = sides(2 * half * ROWS, 2 * ROWS)
        for side in range(3):
            block = 2 * side + half
            out = planes[side] + scatter_block(surf[block], incs[side][4 * half : 4 * half + 4])
            cur[2 * block] = out[:ROWS]
            cur[2 * block + 1] = out[ROWS:]
    run_steps(cur, nxt, coef)
    finish(flts, cur, coef, surf, flux, keep, export, full)


def sum_parts(parts):
    lanes = [parts[i] for i in range(4)]
    for i in range(4, parts.shape[0]):
        lanes[i % 4] = lanes[i % 4] + parts[i]
    return (lanes[0] + lanes[1]) + (lanes[2] + lanes[3])


def last_kernel(flts, parts, own, surf, field, interface, work):
    core = lax.axis_index("sub") & 1
    total = sum_parts(parts)
    interface[...] = total.reshape(2, 512)
    temps = own[pl.ds(4 * ROWS, 8), :]
    temps = jnp.where(core == 0, temps[:4], temps[4:])
    inc = flts[0:1, :] * (total[:4] - temps) + flts[1:2, :] * total[4:]
    add = scatter_block(surf[pl.ds(2 + core, 1)][0], inc)
    start = pl.multiple_of(core * 2 * ROWS, 2 * ROWS)
    work[...] = own[pl.ds(start, 2 * ROWS), :] + add
    rows = [work[pl.ds(p * ROWS + lane, 16, stride=8), :] for p in range(2) for lane in range(8)]
    field[...] = jnp.concatenate(rows, axis=0).reshape(2, 128 * ROWS)


def patch_kernel(ints, source, place, targets, maps, out, *, final):
    slots = place.shape[0]
    subs = out.shape[0]
    parts = 2 if final else 1
    lanes = [place[pl.ds(8 * w, 8), :] & 127 for w in range(slots // 8)]
    rows = [place[pl.ds(8 * w, 8), :] >> 7 for w in range(slots // 8)]
    vals = [[jnp.zeros((8, 128), F32) for _ in rows] for _ in range(parts)]
    at = jnp.max(ints[0:1, :].astype(F32)).astype(jnp.int32)
    for i in range(3):
        tile = source[(at & -subs) + ((at + i) & (subs - 1))]
        for q in range(parts):
            for j in range(4):
                line = jnp.broadcast_to(tile[4 * q + j : 4 * q + j + 1], (8, 128))
                for w in range(slots // 8):
                    got = jnp.take_along_axis(line, lanes[w], axis=1, mode="promise_in_bounds")
                    vals[q][w] = jnp.where(rows[w] == 4 * i + j, got, vals[q][w])
    columns = []
    for q in range(parts):
        full = jnp.concatenate(vals[q] + [jnp.zeros((128 - slots, 128), F32)], axis=0)
        columns.append(full.T)
    left, right = [], [[] for _ in range(parts)]
    for s in range(slots):
        aim = targets[s : s + 1, :]
        left.append(one_hot(aim >> 7, 128))
        table = maps[s]
        for q in range(parts):
            value = jnp.sum(table * columns[q][:, s : s + 1], axis=0, keepdims=True)
            right[q].append(spread(aim & 127, value))
    sums = [product(left, right[q]) for q in range(parts)]
    chips = out.shape[0] // 2
    for c in range(chips):
        if final:
            for k in range(2):
                r = 2 * c + k
                out[r] = jnp.concatenate([s[4 * r : 4 * r + 4] for s in sums], axis=0)
        else:
            for side in range(3):
                n = c + side - 1
                piece = sums[0][8 * n : 8 * n + 8] if 0 <= n < chips else jnp.zeros((8, 128), F32)
                for k in range(2):
                    out[2 * c + k, pl.ds(8 * side, 8), :] = piece


def call(kernel, ins, outs, scratch=()):
    where = {"s": SMEM, "v": VMEM}
    return pl.pallas_call(
        kernel,
        out_shape=[jax.ShapeDtypeStruct(s, d) for s, d, _ in outs],
        in_specs=[pl.BlockSpec(memory_space=where[i]) for i in ins],
        out_specs=[pl.BlockSpec(memory_space=where[o]) for _, _, o in outs],
        scratch_shapes=[pltpu.VMEM(s, F32) for s in scratch],
        compiler_params=pltpu.CompilerParams(vmem_limit_bytes=16 * 1024 * 1024),
    )


def local(
    initial_field,
    conduct,
    velocity,
    heat_release,
    group_kind,
    partner,
    surface_cell,
    patch_count,
    patch_centres,
    patch_targets,
    patch_maps,
):
    subs = lax.axis_size("sub")
    groups = lax.axis_size("grp")
    block = surface_cell.shape[1]
    slots = patch_maps.shape[1]
    planes, cells = initial_field.shape[1:]

    fields = jnp.concatenate([initial_field, conduct, velocity, heat_release], axis=0)
    (payload,) = call(pack_kernel, "vv", [((1032, 128), F32, "v")])(fields, surface_cell)
    swap = [(i, i ^ 1) for i in range(subs)]
    cross = [(i, i + 1 if i % 2 else i - 1) for i in range(1, subs - 1)]
    near = lax.ppermute(payload, "sub", cross)
    mate = lax.ppermute(payload, "sub", swap)
    (far,) = call(far_kernel, "v", [((5 * ROWS + 8, 128), F32, "v")])(mate)
    far = lax.ppermute(far, "sub", cross)
    ints, flts, place, turned = call(
        prepare_kernel,
        "sssvv",
        [
            ((8, 128), jnp.int32, "v"),
            ((8, 128), F32, "v"),
            ((slots, 128), jnp.int32, "v"),
            ((slots, 128, 128), F32, "v"),
        ],
    )(group_kind, partner, patch_count, patch_centres[0], patch_maps[0])
    targets = patch_targets[0]
    near_other = lax.ppermute(near, "sub", swap)
    far_other = lax.ppermute(far, "sub", swap)

    keep_out = ((4 * ROWS + 8, 128), F32, "v")
    half_out = ((groups * subs, 4, 128), F32, "v")
    full_out = ((groups * subs, 8, 128), F32, "v")
    coef_shape = (4, WIDE - 2, ROWS, 128)
    work = [(WIDE, ROWS, 128), (WIDE, ROWS, 128), (2 * ROWS, 128)]
    keep, send, coef, surf = call(
        first_kernel,
        "vvvvvvv",
        [keep_out, half_out, (coef_shape, F32, "v"), ((6, 4, 128), jnp.int32, "v")],
        work,
    )(flts, payload, mate, near, near_other, far, far_other)
    for iteration in range(COUPLE):
        final = iteration == COUPLE - 1
        if not final:
            beside = lax.ppermute(keep, "sub", cross)
        source = lax.all_to_all(send, ("grp", "sub"), 0, 0, tiled=True)
        if not final:
            source, beside = lax.optimization_barrier((source, beside))
            other = lax.ppermute(beside, "sub", swap)
        (parts,) = call(
            functools.partial(patch_kernel, final=final),
            "vvvvv",
            [((subs, 8 if final else 24, 128), F32, "v")],
        )(ints, source, place, targets, turned)
        if not final:
            parts, other = lax.optimization_barrier((parts, other))
        parts = lax.all_to_all(parts, "sub", 0, 0, tiled=True)
        if final:
            field, interface = call(
                last_kernel,
                "vvvv",
                [((planes, cells), F32, "v"), ((2, block), F32, "v")],
                [(2 * ROWS, 128)],
            )(flts, parts, keep, surf)
        else:
            full = iteration == COUPLE - 2
            keep, send = call(
                functools.partial(middle_kernel, full=full),
                "vvvvvvv",
                [keep_out, full_out if full else half_out],
                work,
            )(flts, parts, keep, beside, other, surf, coef)
    return field[None], interface[None]


def solution(mesh):
    placed = (
        P("grp", "sub", None),
        P("grp", "sub", None),
        P("grp", "sub", None),
        P("grp", "sub", None),
        P(),
        P(),
        P("grp", "sub"),
        P("grp", None),
        P("grp", "sub", None),
        P("grp", "sub", None),
        P("grp", "sub", None, None),
    )
    return jax.shard_map(
        local,
        mesh=mesh,
        in_specs=placed,
        out_specs=(P("grp", "sub", None), P("grp", None, "sub")),
        check_vma=False,
    )
```
